1024 devices in a mesh: seq: 16 (over y, x), rep: 64 (over z, core).
Axes of the slice: x: 4, y: 4, z: 32, core: 2. Of those that a mesh axis runs over, the one named last changes fastest.
Arguments:
- mixer_in: bfloat16 [64, 2048, 4096], P('rep', 'seq'), may hold values from -6 to 6
- write_proj: bfloat16 [64, 2048, 512], P('rep', 'seq'), may hold values from -6 to 6
- read_proj: bfloat16 [64, 2048, 512], P('rep', 'seq'), may hold values from -0.5 to 0.5
- dt_steps: int32 [64, 2048, 64], P('rep', 'seq'), may hold values from 1 to 16
- decay_exp: int32 [64, 2048, 64], P('rep', 'seq'), may hold values from 1 to 50000, as said below
- norm_gain: float32 [4096], P('seq'), may hold values from 0.1 to 1.9
- skip_gain: float32 [64], P('seq'), may hold values from 1 to 4
- out_grad: bfloat16 [64, 2048, 4096], P('rep', 'seq'), may hold values from -80 to 80
Outputs:
- mixer_grad: bfloat16 [64, 2048, 4096], P('rep', 'seq')
- read_grad: bfloat16 [64, 2048, 512], P('rep', 'seq')
- gain_grad: float32 [4096], P('seq')
- skip_grad: float32 [64], P('seq')
The draws below stay inside these ranges and needn't reach their ends.
Inputs may be any that keep to these rules, and one draw needn't show every extreme that they name: The decay factor of head h at position t is exp(-decay_exp / 65536).
All inputs are finite; a program needn't handle non-finite values.
Results may differ from the reference program's by a relative error of at most 0.015.
Values may be sent and summed in bfloat16 or wider, within the bound.
No kernel may reach another device: no remote copies, remote signals or barrier semaphores. Data moves between devices by JAX's collectives and lax.ppermute only.
A program may use at most 64 MiB of HBM per device.

```python
from functools import partial
import jax
import jax.numpy as jnp
from jax import lax

H = 64
P_SIZE = 64
N = 128
G = 4
HG = 16
L_DEV = 128
SEQLEN = 2048
BATCH = 64
N_SEQ = 16


def draw_decay_exp(key, part):
    keys = jax.random.split(key, 8)
    blocks = SEQLEN // L_DEV
    mixed_group = jax.random.randint(keys[0], (BATCH, 1, G, 1), 0, 2)
    mixed_head = jnp.broadcast_to(mixed_group, (BATCH, 1, G, HG)).reshape(BATCH, 1, 1, H)
    quick_turn = jax.random.randint(keys[7], (BATCH, blocks, 1, H), 0, 3)
    quick_block = mixed_head * (quick_turn == 0).astype(jnp.int32)
    slow_unit = max(32768 // SEQLEN // 6, 1)
    magnitude = jax.random.randint(keys[1], (BATCH, blocks, 1, H), 1, 5)
    quick_factor = 1 + (magnitude + 1) // 2
    per_block = jnp.where(quick_block == 1, 256 * quick_factor, slow_unit * magnitude)
    per_block = jnp.broadcast_to(per_block, (BATCH, blocks, L_DEV, H)).reshape(BATCH, SEQLEN, H)
    stochastic_perturbation = jax.random.randint(keys[2], (BATCH, SEQLEN, H), 1, 5)
    front_displacement = jax.random.randint(keys[3], (BATCH, 1, H), 0, SEQLEN // 2)
    rear_displacement = jax.random.randint(keys[4], (BATCH, 1, H), SEQLEN // 2, SEQLEN)
    front_extent = jax.random.randint(keys[5], (BATCH, 1, H), 14600, 45400)
    rear_extent = jax.random.randint(keys[6], (BATCH, 1, H), 14600, 45400)
    element_indices = jnp.arange(SEQLEN)[None, :, None]
    pulse_clusters = jnp.where(element_indices == front_displacement, front_extent, 0) + jnp.where(element_indices == rear_displacement, rear_extent, 0)
    pulse_clusters = pulse_clusters * (1 - mixed_head.reshape(BATCH, 1, H))
    return (per_block * stochastic_perturbation + pulse_clusters).astype(jnp.int32)


def draw_out_grad(key, part):
    position = jnp.arange(SEQLEN, dtype=jnp.float32) / SEQLEN
    sequence = jnp.arange(BATCH, dtype=jnp.float32) / BATCH
    scale = (1.0 + 2.0 * position)[None, :, None] * (1.0 + 2.0 * sequence)[:, None, None]
    values = jnp.clip(jax.random.normal(key, (BATCH, SEQLEN, H * P_SIZE), jnp.float32), -4.0, 4.0) * scale
    return values.astype(jnp.bfloat16)


def plant(array, stream_key, smallest, largest):
    extent = array.shape
    place = [jax.random.randint(jax.random.fold_in(stream_key, axis), (), 0, extent[axis]) for axis in range(len(extent))]
    array = array.at[tuple(place)].set(smallest)
    longest = extent.index(max(extent))
    place[longest] = (place[longest] + 1) % extent[longest]
    return array.at[tuple(place)].set(largest)


def block_levels(stream_key, extent, cuts, low, high):
    factor_of = 1.0
    for dim, shards_of in cuts:
        heights = jax.random.uniform(jax.random.fold_in(jax.random.fold_in(stream_key, 6), dim), (shards_of,), jnp.float32, low / len(cuts), high / len(cuts))
        factor_of = factor_of * jnp.repeat(jnp.exp(heights), extent[dim] // shards_of).reshape((-1,) + (1,) * (len(extent) - 1 - dim))
    return factor_of


def gaussian(own_key, shape, deviation, reach, cuts=(), kind=jnp.bfloat16):
    values = jax.random.normal(own_key, shape, jnp.float32) * deviation
    if len(cuts) > 0:
        values = block_levels(own_key, shape, cuts, -0.22, 0.18) * values
    return jnp.clip(values, min=-reach, max=reach).astype(kind)


def setup_inputs(seed: int = 0) -> dict:
    arg_keys = jax.random.split(jax.random.key(seed), 9)
    return {
        "mixer_in": gaussian(arg_keys[0], (BATCH, SEQLEN, H * P_SIZE), 1.0, 6.0, ((0, 64), (1, 16))),
        "write_proj": gaussian(arg_keys[1], (BATCH, SEQLEN, G * N), 1.0, 6.0, ((0, 64), (1, 16))),
        "read_proj": gaussian(arg_keys[2], (BATCH, SEQLEN, G * N), N ** -0.5, 0.5, ((0, 64), (1, 16))),
        "dt_steps": plant(jax.random.randint(arg_keys[3], (BATCH, SEQLEN, H), 1, 17), jax.random.fold_in(arg_keys[3], 1), 1, 16).astype(jnp.int32),
        "decay_exp": draw_decay_exp(jax.random.fold_in(arg_keys[8], 71), 0),
        "norm_gain": jnp.clip(1.0 + 0.18 * jax.random.normal(arg_keys[5], (H * P_SIZE,), jnp.float32), 0.1, 1.9),
        "skip_gain": jnp.clip(1.0 + 3.0 * jax.random.uniform(arg_keys[6], (H,), jnp.float32) ** block_levels(arg_keys[6], (H,), ((0, 16),), -0.2, 0.2), 1.0, 4.0),
        "out_grad": draw_out_grad(jax.random.fold_in(arg_keys[8], 71), 0),
    }


def contract(form, left, right):
    return jnp.einsum(form, left.astype(jnp.float32), right.astype(jnp.float32))

def block_front(mixed, write, read, steps, decay):
    length = mixed.shape[0]
    log_decay = -(jnp.cumsum(jnp.transpose(decay).reshape(G, HG, length), axis=2).astype(jnp.float32) / 65536.0)
    step_size = jnp.transpose(steps).reshape(G, HG, length).astype(jnp.float32) / 16.0
    causal = jnp.arange(length)[:, None] >= jnp.arange(length)[None, :]
    spread = jnp.where(causal, log_decay[:, :, :, None] - log_decay[:, :, None, :], 0.0)
    weights = jnp.where(causal, jnp.exp(spread), 0.0) * step_size[:, :, None, :]
    scores = contract('tgn,sgn->gts', read, write)
    mixing = (scores[:, None] * weights).astype(jnp.bfloat16)
    inner_part = contract('gjts,sgjp->tgjp', mixing, mixed)
    ending = jnp.transpose(jnp.exp(log_decay[:, :, -1:] - log_decay) * step_size, (2, 0, 1))
    weighted = (mixed.astype(jnp.float32) * ending[..., None]).astype(jnp.bfloat16)
    span_state = contract('sgjp,sgn->gjpn', weighted, write).astype(jnp.bfloat16)
    block_decay = jnp.exp(log_decay[:, :, -1]).astype(jnp.bfloat16)
    readout = jnp.transpose(jnp.exp(log_decay), (2, 0, 1))
    return (weights, mixing, inner_part, ending, weighted, span_state, block_decay, readout)

def block_middle(mixed, read, skip_full, gain_full, upstream, inner_part, readout, carried):
    mixed_wide = mixed.astype(jnp.float32)
    mixer_out = inner_part + readout[..., None] * contract('tgn,gjpn->tgjp', read, carried) + skip_full[None, :, :, None] * mixed_wide
    inverse = lax.rsqrt(lax.optimization_barrier(jnp.mean(mixer_out * mixer_out, axis=(2, 3), keepdims=True)) + 1e-05)
    normed = mixer_out * inverse
    upstream_wide = upstream.astype(jnp.float32)
    normed_grad = upstream_wide * gain_full[None]
    gain_part = lax.optimization_barrier(jnp.sum(upstream_wide * normed, axis=0))
    delta_wide = inverse * (normed_grad - normed * lax.optimization_barrier(jnp.mean(normed_grad * normed, axis=(2, 3), keepdims=True)))
    skip_part = lax.optimization_barrier(jnp.sum(delta_wide * mixed_wide, axis=(0, 3)))
    delta_half = delta_wide.astype(jnp.bfloat16)
    scaled_delta = (delta_wide * readout[..., None]).astype(jnp.bfloat16)
    state_grad = contract('tgjp,tgn->gjpn', scaled_delta, read).astype(jnp.bfloat16)
    read_part = contract('tgjp,gjpn->tgn', scaled_delta, carried)
    return (delta_wide, delta_half, state_grad, read_part, gain_part, skip_part)

def block_back(mixed, write, skip_full, weights, mixing, ending, delta_wide, delta_half, read_part, carried_grad):
    mix_grad = contract('tgjp,sgjp->gjts', delta_half, mixed)
    score_grad = lax.optimization_barrier(jnp.sum(mix_grad * weights, axis=1)).astype(jnp.bfloat16)
    read_grad = contract('gts,sgn->tgn', score_grad, write) + read_part
    mixer_grad = contract('gjts,tgjp->sgjp', mixing, delta_half)
    mixer_grad = mixer_grad + ending[..., None] * contract('sgn,gjpn->sgjp', write, carried_grad)
    mixer_grad = mixer_grad + skip_full[None, :, :, None] * delta_wide
    return (mixer_grad.astype(jnp.bfloat16), read_grad.astype(jnp.bfloat16))

def forward_step(carry, item):
    decay_now, state_now = item
    updated = (decay_now.astype(jnp.float32)[..., None, None] * carry.astype(jnp.float32) + state_now.astype(jnp.float32)).astype(jnp.bfloat16)
    return (updated, carry)

def backward_step(carry, item):
    decay_now, grad_now = item
    updated = (grad_now.astype(jnp.float32) + decay_now.astype(jnp.float32)[..., None, None] * carry.astype(jnp.float32)).astype(jnp.bfloat16)
    return (updated, carry)

def one_sequence(pieces, gain_full, skip_full):
    mixed, write, read, steps, decay, upstream = pieces
    blocks = N_SEQ
    mixed = mixed.reshape(blocks, L_DEV, G, HG, P_SIZE)
    upstream = upstream.reshape(blocks, L_DEV, G, HG, P_SIZE)
    write = write.reshape(blocks, L_DEV, G, N)
    read = read.reshape(blocks, L_DEV, G, N)
    steps = steps.reshape(blocks, L_DEV, H)
    decay = decay.reshape(blocks, L_DEV, H)
    weights, mixing, inner_part, ending, weighted, span_state, block_decay, readout = jax.vmap(block_front)(mixed, write, read, steps, decay)
    start = jnp.zeros((G, HG, P_SIZE, N), jnp.bfloat16)
    final_state, carried = lax.scan(forward_step, start, (block_decay, span_state))
    middle = jax.vmap(block_middle, in_axes=(0, 0, None, None, 0, 0, 0, 0))(mixed, read, skip_full, gain_full, upstream, inner_part, readout, carried)
    delta_wide, delta_half, state_grad, read_part, gain_part, skip_part = middle
    first_grad, carried_grad = lax.scan(backward_step, start, (block_decay, state_grad), reverse=True)
    mixer_grad, read_grad = jax.vmap(block_back, in_axes=(0, 0, None, 0, 0, 0, 0, 0, 0, 0))(mixed, write, skip_full, weights, mixing, ending, delta_wide, delta_half, read_part, carried_grad)
    return (mixer_grad.reshape(SEQLEN, H * P_SIZE), read_grad.reshape(SEQLEN, G * N), lax.optimization_barrier(jnp.sum(gain_part, axis=0)), lax.optimization_barrier(jnp.sum(skip_part, axis=0)))

def reference(mixer_in, write_proj, read_proj, dt_steps, decay_exp, norm_gain, skip_gain, out_grad):
    gain_full = norm_gain.reshape(G, HG, P_SIZE)
    skip_full = skip_gain.reshape(G, HG)
    runner = partial(one_sequence, gain_full=gain_full, skip_full=skip_full)
    mixer_grad, read_grad, gain_parts, skip_parts = lax.map(runner, (mixer_in, write_proj, read_proj, dt_steps, decay_exp, out_grad))
    return (mixer_grad, read_grad, lax.optimization_barrier(jnp.sum(gain_parts, axis=0)).reshape(H * P_SIZE), lax.optimization_barrier(jnp.sum(skip_parts, axis=0)).reshape(H))
```

```python
import jax
import jax.numpy as jnp
from jax import lax
from jax.experimental import pallas as pl
from jax.experimental.pallas import tpu as pltpu
from jax.sharding import Mesh
from jax.sharding import PartitionSpec as P

H = 64
P_SIZE = 64
N = 128
G = 4
HG = 16
T = 128
D = 16
HEADS = H // D
LANES = HEADS * P_SIZE
SEQ = ("seq_0", "seq_1")
F32 = jnp.float32
BF16 = jnp.bfloat16
BLOCKS_PER_STEP = 2
STEPS = D // BLOCKS_PER_STEP
FAR = -1e30


def contract(left, right, dims):
    return lax.dot_general(left, right, (dims, ((), ())), preferred_element_type=F32)


def pack_kernel(x_ref, up_ref, write_ref, read_ref, dt_ref, dec_ref, out_ref):
    dec = dec_ref[...]
    high = (dec >> 8).astype(F32)
    low = (dec & 255).astype(F32)
    steps = dt_ref[...].astype(F32)
    for j in range(4):
        cols = slice(LANES * j, LANES * (j + 1))
        out_ref[j, :T, :256] = x_ref[:, cols]
        out_ref[j, :T, 256:512] = up_ref[:, cols]
        out_ref[j, :T, 512:640] = write_ref[...]
        out_ref[j, :T, 640:768] = read_ref[...]
        base = 8 * (j // 2)
        for place, rows in enumerate((steps, high, low)):
            eight = rows[base : base + 8]
            if j % 2 == 1:
                eight = pltpu.roll(eight, 4, 0)
            out_ref[j, T:, 128 * place : 128 * (place + 1)] = eight.astype(BF16)
        out_ref[j, T:, 384:] = jnp.zeros((8, 384), BF16)


def scalars(tail):
    upto = (
        lax.broadcasted_iota(jnp.int32, (T, T), 0) <= lax.broadcasted_iota(jnp.int32, (T, T), 1)
    ).astype(F32).astype(BF16)
    step = tail[:, :128].astype(F32) / 16.0
    whole = contract(tail[:, 128:256], upto, ((1,), (0,))) * 256.0 + contract(
        tail[:, 256:384], upto, ((1,), (0,))
    )
    log_decay = -(whole / 65536.0)
    last = jnp.broadcast_to(log_decay[:, T - 1 : T], (8, T))
    ending = jnp.exp(last - log_decay) * step
    readout = jnp.exp(log_decay)
    block_decay = jnp.exp(last).astype(BF16).astype(F32)
    cols = jnp.transpose(jnp.concatenate([log_decay, step, ending, readout], axis=0))
    return log_decay, step, block_decay, cols


def low_half(shape):
    return lax.broadcasted_iota(jnp.int32, shape, len(shape) - 1) < P_SIZE


def spread(cols, at):
    mask = low_half((T, 128))
    pairs = []
    for i in range(HEADS // 2):
        a = jnp.broadcast_to(cols[:, at + 2 * i : at + 2 * i + 1], (T, 128))
        b = jnp.broadcast_to(cols[:, at + 2 * i + 1 : at + 2 * i + 2], (T, 128))
        pairs.append(jnp.where(mask, a, b))
    return jnp.concatenate(pairs, axis=1)


def spread_rows(rows):
    mask = low_half((1, 128))
    return jnp.concatenate(
        [
            jnp.where(mask, rows[2 * i : 2 * i + 1], rows[2 * i + 1 : 2 * i + 2])
            for i in range(HEADS // 2)
        ],
        axis=1,
    )


def skip_lanes(skip_ref):
    lane = lax.broadcasted_iota(jnp.int32, (1, LANES), 1) // P_SIZE
    row = jnp.full((1, LANES), skip_ref[HEADS - 1], F32)
    for j in range(HEADS - 1):
        row = jnp.where(lane == j, skip_ref[j], row)
    return row


def two_heads(pair):
    mask = low_half((T, 128))
    return jnp.concatenate(
        [jnp.where(mask, pair, 0.0).astype(BF16), jnp.where(mask, 0.0, pair).astype(BF16)], axis=0
    )


def forward_kernel(in_ref, gain_ref, skip_ref, mo_ref, carried_ref, stats_ref, carry, sums):
    step_id = pl.program_id(0)

    @pl.when(step_id == 0)
    def _():
        carry[...] = jnp.zeros_like(carry)
        sums[...] = jnp.zeros_like(sums)

    gain = gain_ref[...]
    skip = skip_lanes(skip_ref)
    row_id = lax.broadcasted_iota(jnp.int32, (T, T), 0)
    lane_id = lax.broadcasted_iota(jnp.int32, (T, T), 1)
    causal = row_id >= lane_id
    state = carry[...]
    found = sums[...]
    results = []
    for b in range(BLOCKS_PER_STEP):
        x = in_ref[b, :T, :256].astype(F32)
        up = in_ref[b, :T, 256:512].astype(F32)
        write = in_ref[b, :T, 512:640]
        read = in_ref[b, :T, 640:768]
        log_decay, step, block_decay, cols = scalars(in_ref[b, T:, :])
        scores = contract(read, write, ((1,), (1,)))
        inner = []
        for i in range(HEADS // 2):
            mixing = []
            for j in (2 * i, 2 * i + 1):
                gap = jnp.where(causal, cols[:, j : j + 1] - log_decay[j : j + 1], FAR)
                mixing.append((scores * (jnp.exp(gap) * step[j : j + 1])).astype(BF16))
            inner.append(
                contract(
                    jnp.concatenate(mixing, axis=1),
                    two_heads(x[:, 128 * i : 128 * (i + 1)]),
                    ((1,), (0,)),
                )
            )
        weighted = (x * spread(cols, 16)).astype(BF16)
        span_state = contract(write, weighted, ((0,), (0,))).astype(BF16).astype(F32)
        carried = state.astype(BF16)
        state = (spread_rows(block_decay) * state + span_state).astype(BF16).astype(F32)
        out = (
            jnp.concatenate(inner, axis=1)
            + spread(cols, 24) * contract(read, carried, ((1,), (0,)))
            + skip * x
        )
        square = jnp.sum(out * out, axis=1, keepdims=True)
        cross = jnp.sum(up * gain * out, axis=1, keepdims=True)
        at = 2 * (BLOCKS_PER_STEP * step_id + b)
        found = jnp.where(lane_id == at, square, jnp.where(lane_id == at + 1, cross, found))
        results.append((out, carried))
    for b, (out, carried) in enumerate(results):
        mo_ref[b] = out
        carried_ref[b] = carried
    carry[...] = state
    sums[...] = found

    @pl.when(step_id == STEPS - 1)
    def _():
        rows = jnp.transpose(sums[...])[: 2 * D]
        for d in range(4):
            stats_ref[d] = rows


def backward_kernel(
    in_ref, mo_ref, carried_ref, stats_ref, gain_ref, skip_ref, out_ref, part_ref, carry, sums, parts
):
    step_id = pl.program_id(0)

    @pl.when(step_id == 0)
    def _():
        carry[...] = jnp.zeros_like(carry)
        parts[...] = jnp.zeros_like(parts)
        total = stats_ref[0] + stats_ref[1] + stats_ref[2] + stats_ref[3]
        sums[...] = jnp.transpose(jnp.concatenate([total] * 4, axis=0))

    gain = gain_ref[...]
    skip = skip_lanes(skip_ref)
    row_id = lax.broadcasted_iota(jnp.int32, (T, T), 0)
    lane_id = lax.broadcasted_iota(jnp.int32, (T, T), 1)
    later = row_id <= lane_id
    state = carry[...]
    gain_sum = parts[0:1]
    skip_sum = parts[1:2]
    results = []
    first = BLOCKS_PER_STEP * (STEPS - 1 - step_id)
    found = sums[...]
    for b in reversed(range(BLOCKS_PER_STEP)):
        x = in_ref[b, :T, :256].astype(F32)
        up = in_ref[b, :T, 256:512].astype(F32)
        write = in_ref[b, :T, 512:640]
        read = in_ref[b, :T, 640:768]
        out = mo_ref[b]
        log_decay, step, block_decay, cols = scalars(in_ref[b, T:, :])
        here = pltpu.roll(found, lax.rem(128 - 2 * (first + b), 128), 1)
        inverse = lax.rsqrt(here[:, 0:1] / (HG * P_SIZE) + 1e-05)
        mean = inverse * here[:, 1:2] / (HG * P_SIZE)
        normed = out * inverse
        delta = inverse * (up * gain - normed * mean)
        gain_sum = gain_sum + jnp.sum(up * normed, axis=0, keepdims=True)
        skip_sum = skip_sum + jnp.sum(delta * x, axis=0, keepdims=True)
        scaled = (delta * spread(cols, 24)).astype(BF16)
        half = delta.astype(BF16)
        scores = contract(write, read, ((1,), (1,)))
        score_grad = jnp.zeros((T, T), F32)
        mixed = []
        for i in range(HEADS // 2):
            pair = slice(128 * i, 128 * (i + 1))
            mix_grad = contract(two_heads(x[:, pair]), half[:, pair], ((1,), (1,)))
            mixing = []
            for n, j in enumerate((2 * i, 2 * i + 1)):
                gap = jnp.where(later, log_decay[j : j + 1] - cols[:, j : j + 1], FAR)
                weight = jnp.exp(gap) * cols[:, 8 + j : 9 + j]
                mixing.append((scores * weight).astype(BF16))
                score_grad = score_grad + weight * mix_grad[T * n : T * (n + 1)]
            mixed.append(
                contract(
                    jnp.concatenate(mixing, axis=1), two_heads(delta[:, pair]), ((1,), (0,))
                )
            )
        carried_grad = state.astype(BF16)
        mixer_grad = (
            jnp.concatenate(mixed, axis=1)
            + spread(cols, 16) * contract(write, carried_grad, ((1,), (0,)))
            + skip * delta
        )
        read_grad = contract(score_grad.astype(BF16), write, ((0,), (0,))) + contract(
            scaled, carried_ref[b], ((1,), (1,))
        )
        state_grad = contract(read, scaled, ((0,), (0,))).astype(BF16).astype(F32)
        state = (state_grad + spread_rows(block_decay) * state).astype(BF16).astype(F32)
        results.append((b, mixer_grad, read_grad))
    for b, mixer_grad, read_grad in results:
        out_ref[b, :, :256] = mixer_grad.astype(BF16)
        out_ref[b, :, 256:] = read_grad.astype(BF16)
    carry[...] = state
    parts[0:1] = gain_sum
    parts[1:2] = skip_sum

    @pl.when(step_id == STEPS - 1)
    def _():
        part_ref[0:1] = parts[0:1]
        part_ref[1:2] = parts[1:2]


def unpack_kernel(in_ref, mixer_ref, read_ref):
    total = jnp.zeros((T, 128), F32)
    for j in range(4):
        mixer_ref[:, LANES * j : LANES * (j + 1)] = in_ref[j, :, :256]
        total = total + in_ref[j, :, 256:].astype(F32)
    read_ref[...] = total.astype(BF16)


def whole(shape):
    return pl.BlockSpec(shape, lambda i: (0,) * len(shape))


SCALARS = pl.BlockSpec(memory_space=pltpu.SMEM)


def call(kernel, grid, in_specs, out_specs, out_shape, scratch=(), flops=0, interpret=False):
    return pl.pallas_call(
        kernel,
        grid=(grid,),
        in_specs=in_specs,
        out_specs=out_specs,
        out_shape=out_shape,
        scratch_shapes=scratch,
        cost_estimate=pl.CostEstimate(flops=flops, bytes_accessed=1 << 20, transcendentals=0),
        interpret=interpret,
    )


def shape(dims, dtype):
    return jax.ShapeDtypeStruct(dims, dtype)


def build(interpret):
    def on_device(mixer_in, write_proj, read_proj, dt_steps, decay_exp, norm_gain, skip_gain, out_grad):
        def exchange(array, axes):
            return lax.all_to_all(array, axes, split_axis=0, concat_axis=0, tiled=True)

        gain = norm_gain.reshape(1, LANES)
        column = lambda i: (0, i)
        sent = call(
            pack_kernel,
            G,
            [
                pl.BlockSpec((T, 1024), column),
                pl.BlockSpec((T, 1024), column),
                pl.BlockSpec((T, N), column),
                pl.BlockSpec((T, N), column),
                pl.BlockSpec((HG, T), lambda i: (i, 0)),
                pl.BlockSpec((HG, T), lambda i: (i, 0)),
            ],
            pl.BlockSpec((4, T + 8, 768), lambda i: (i, 0, 0)),
            shape((D, T + 8, 768), BF16),
            interpret=interpret,
        )(
            mixer_in[0],
            out_grad[0],
            write_proj[0],
            read_proj[0],
            jnp.transpose(dt_steps[0]),
            jnp.transpose(decay_exp[0]),
        )
        blocks = exchange(sent, SEQ)

        along = lambda i: (i, 0, 0)
        size = BLOCKS_PER_STEP
        mixer_out, carried, stats = call(
            forward_kernel,
            STEPS,
            [pl.BlockSpec((size, T + 8, 768), along), whole((1, LANES)), SCALARS],
            [
                pl.BlockSpec((size, T, LANES), along),
                pl.BlockSpec((size, N, LANES), along),
                whole((4, 2 * D, T)),
            ],
            [
                shape((D, T, LANES), F32),
                shape((D, N, LANES), BF16),
                shape((4, 2 * D, T), F32),
            ],
            [pltpu.VMEM((N, LANES), F32), pltpu.VMEM((T, T), F32)],
            interpret=interpret,
        )(blocks, gain, skip_gain)
        stats = exchange(stats, "seq_1")

        back = lambda i: (STEPS - 1 - i, 0, 0)
        grads, parts = call(
            backward_kernel,
            STEPS,
            [
                pl.BlockSpec((size, T + 8, 768), back),
                pl.BlockSpec((size, T, LANES), back),
                pl.BlockSpec((size, N, LANES), back),
                whole((4, 2 * D, T)),
                whole((1, LANES)),
                SCALARS,
            ],
            [pl.BlockSpec((size, T, 384), back), whole((2, LANES))],
            [shape((D, T, 384), BF16), shape((2, LANES), F32)],
            [pltpu.VMEM((N, LANES), F32), pltpu.VMEM((T, T), F32), pltpu.VMEM((8, LANES), F32)],
            interpret=interpret,
        )(blocks, mixer_out, carried, stats, gain, skip_gain)
        grads = exchange(grads, SEQ)

        for axis in ("core", "z_low"):
            if lax.axis_size(axis) == 2:
                parts = parts + lax.ppermute(parts, axis, [(0, 1), (1, 0)])
        far = lax.axis_size("z_high")
        if far > 1:
            copies = jnp.broadcast_to(parts[None], (far, 2, LANES))
            parts = jnp.sum(exchange(copies, "z_high"), axis=0)
        mixer_grad, read_grad = call(
            unpack_kernel,
            G,
            [pl.BlockSpec((4, T, 384), along)],
            [pl.BlockSpec((T, 1024), column), pl.BlockSpec((T, N), column)],
            [shape((T, H * P_SIZE), BF16), shape((T, G * N), BF16)],
            interpret=interpret,
        )(grads)
        return (
            mixer_grad[None],
            read_grad[None],
            parts[0],
            jnp.sum(parts[1].reshape(HEADS, P_SIZE), axis=1),
        )

    return on_device


def sharded(mesh, interpret=False):
    rep = ("z_high", "z_low", "core")
    big = P(rep, SEQ, None)
    return jax.shard_map(
        build(interpret),
        mesh=mesh,
        in_specs=(big, big, big, big, big, P(SEQ), P(SEQ), big),
        out_specs=(big, big, P(SEQ), P(SEQ)),
        check_vma=False,
    )


def solution(mesh):
    names = ("seq_0", "seq_1", "z_high", "z_low", "core")
    return sharded(Mesh(mesh.devices.reshape(4, 4, 16, 2, 2), names))
```

```python
import jax
import jax.numpy as jnp
from jax import lax
from jax.experimental import pallas as pl
from jax.experimental.pallas import tpu as pltpu
from jax.sharding import Mesh
from jax.sharding import PartitionSpec as P


H = 64
P_SIZE = 64
N = 128
G = 4
HG = 16
T = 128
D = 16
HEADS = H // D
LANES = HEADS * P_SIZE
SEQ = ("seq_0", "seq_1")
F32 = jnp.float32
BF16 = jnp.bfloat16
BLOCKS_PER_STEP = 2
STEPS = D // BLOCKS_PER_STEP
PACK_STEPS = 2
GAIN_BLOCKS = 4
FAR = -1e30


def contract(left, right, dims):
    return lax.dot_general(left, right, (dims, ((), ())), preferred_element_type=F32)


def pack_kernel(x_ref, up_ref, write_ref, read_ref, dt_ref, dec_ref, out_ref):
    dec = dec_ref[...]
    high = (dec >> 8).astype(F32)
    low = (dec & 255).astype(F32)
    steps = dt_ref[...].astype(F32)
    for j in range(D // PACK_STEPS):
        cols = slice(LANES * j, LANES * (j + 1))
        group = slice(N * (j // 4), N * (j // 4 + 1))
        out_ref[j, :T, :256] = x_ref[:, cols]
        out_ref[j, :T, 256:512] = up_ref[:, cols]
        out_ref[j, :T, 512:640] = write_ref[:, group]
        out_ref[j, :T, 640:768] = read_ref[:, group]
        base = 8 * (j // 2)
        for place, rows in enumerate((steps, high, low)):
            eight = rows[base : base + 8]
            if j % 2 == 1:
                eight = pltpu.roll(eight, 4, 0)
            out_ref[j, T:, 128 * place : 128 * (place + 1)] = eight.astype(BF16)
        out_ref[j, T:, 384:] = jnp.zeros((8, 384), BF16)


def scalars(tail):
    upto = (
        lax.broadcasted_iota(jnp.int32, (T, T), 0) <= lax.broadcasted_iota(jnp.int32, (T, T), 1)
    ).astype(F32).astype(BF16)
    step = tail[:, :128].astype(F32) / 16.0
    whole = contract(tail[:, 128:256], upto, ((1,), (0,))) * 256.0 + contract(
        tail[:, 256:384], upto, ((1,), (0,))
    )
    log_decay = -(whole / 65536.0)
    last = jnp.broadcast_to(log_decay[:, T - 1 : T], (8, T))
    ending = jnp.exp(last - log_decay) * step
    readout = jnp.exp(log_decay)
    block_decay = jnp.exp(last).astype(BF16).astype(F32)
    cols = jnp.transpose(jnp.concatenate([log_decay, step, ending, readout], axis=0))
    return log_decay, step, block_decay, cols


def low_half(shape):
    return lax.broadcasted_iota(jnp.int32, shape, len(shape) - 1) < P_SIZE


def spread(cols, at):
    mask = low_half((T, 128))
    pairs = []
    for i in range(HEADS // 2):
        a = jnp.broadcast_to(cols[:, at + 2 * i : at + 2 * i + 1], (T, 128))
        b = jnp.broadcast_to(cols[:, at + 2 * i + 1 : at + 2 * i + 2], (T, 128))
        pairs.append(jnp.where(mask, a, b))
    return jnp.concatenate(pairs, axis=1)


def spread_rows(rows):
    mask = low_half((1, 128))
    return jnp.concatenate(
        [
            jnp.where(mask, rows[2 * i : 2 * i + 1], rows[2 * i + 1 : 2 * i + 2])
            for i in range(HEADS // 2)
        ],
        axis=1,
    )


def skip_lanes(skip_ref):
    lane = lax.broadcasted_iota(jnp.int32, (1, LANES), 1) // P_SIZE
    row = jnp.full((1, LANES), skip_ref[HEADS - 1], F32)
    for j in range(HEADS - 1):
        row = jnp.where(lane == j, skip_ref[j], row)
    return row


def two_heads(pair):
    mask = low_half((T, 128))
    return jnp.concatenate(
        [jnp.where(mask, pair, 0.0).astype(BF16), jnp.where(mask, 0.0, pair).astype(BF16)], axis=0
    )


def forward_kernel(in_ref, gain_ref, skip_ref, mo_ref, carried_ref, stats_ref, carry, sums):
    step_id = pl.program_id(0)

    @pl.when(step_id == 0)
    def _():
        carry[...] = jnp.zeros_like(carry)
        sums[...] = jnp.zeros_like(sums)

    gain = gain_ref[...]
    skip = skip_lanes(skip_ref)
    row_id = lax.broadcasted_iota(jnp.int32, (T, T), 0)
    lane_id = lax.broadcasted_iota(jnp.int32, (T, T), 1)
    causal = row_id >= lane_id
    state = carry[...]
    found = sums[...]
    results = []
    for b in range(BLOCKS_PER_STEP):
        x = in_ref[b, :T, :256].astype(F32)
        up = in_ref[b, :T, 256:512].astype(F32)
        write = in_ref[b, :T, 512:640]
        read = in_ref[b, :T, 640:768]
        log_decay, step, block_decay, cols = scalars(in_ref[b, T:, :])
        scores = contract(read, write, ((1,), (1,)))
        inner = []
        for i in range(HEADS // 2):
            mixing = []
            for j in (2 * i, 2 * i + 1):
                gap = jnp.where(causal, cols[:, j : j + 1] - log_decay[j : j + 1], FAR)
                mixing.append((scores * (jnp.exp(gap) * step[j : j + 1])).astype(BF16))
            inner.append(
                contract(
                    jnp.concatenate(mixing, axis=1),
                    two_heads(x[:, 128 * i : 128 * (i + 1)]),
                    ((1,), (0,)),
                )
            )
        weighted = (x * spread(cols, 16)).astype(BF16)
        span_state = contract(write, weighted, ((0,), (0,))).astype(BF16).astype(F32)
        carried = state.astype(BF16)
        state = (spread_rows(block_decay) * state + span_state).astype(BF16).astype(F32)
        out = (
            jnp.concatenate(inner, axis=1)
            + spread(cols, 24) * contract(read, carried, ((1,), (0,)))
            + skip * x
        )
        square = jnp.sum(out * out, axis=1, keepdims=True)
        cross = jnp.sum(up * gain * out, axis=1, keepdims=True)
        at = 2 * (BLOCKS_PER_STEP * step_id + b)
        found = jnp.where(lane_id == at, square, jnp.where(lane_id == at + 1, cross, found))
        results.append((out, carried))
    for b, (out, carried) in enumerate(results):
        mo_ref[b] = out
        carried_ref[b] = carried
    carry[...] = state
    sums[...] = found

    @pl.when(step_id == STEPS - 1)
    def _():
        rows = jnp.transpose(sums[...])[: 2 * D]
        for d in range(4):
            stats_ref[d] = rows


def shared_sums(stats_ref):
    total = stats_ref[0] + stats_ref[1] + stats_ref[2] + stats_ref[3]
    return jnp.transpose(jnp.concatenate([total] * 4, axis=0))


def normalise(found, block, out, up, gain):
    here = pltpu.roll(found, lax.rem(128 - 2 * block, 128), 1)
    inverse = lax.rsqrt(here[:, 0:1] / (HG * P_SIZE) + 1e-05)
    mean = inverse * here[:, 1:2] / (HG * P_SIZE)
    normed = out * inverse
    return normed, inverse * (up * gain - normed * mean)


def gain_kernel(in_ref, mo_ref, stats_ref, gain_ref, part_ref, sums, parts):
    step_id = pl.program_id(0)

    @pl.when(step_id == 0)
    def _():
        parts[...] = jnp.zeros_like(parts)
        sums[...] = shared_sums(stats_ref)

    gain = gain_ref[...]
    found = sums[...]
    gain_sum = parts[0]
    skip_sum = parts[1]
    for b in range(GAIN_BLOCKS):
        x = in_ref[b, :, :256].astype(F32)
        up = in_ref[b, :, 256:].astype(F32)
        normed, delta = normalise(found, GAIN_BLOCKS * step_id + b, mo_ref[b], up, gain)
        gain_sum = gain_sum + jnp.sum((up * normed).reshape(T // 8, 8, LANES), axis=0)
        skip_sum = skip_sum + jnp.sum((delta * x).reshape(T // 8, 8, LANES), axis=0)
    parts[0] = gain_sum
    parts[1] = skip_sum

    @pl.when(step_id == D // GAIN_BLOCKS - 1)
    def _():
        total = jnp.concatenate(
            [jnp.sum(parts[0], axis=0, keepdims=True), jnp.sum(parts[1], axis=0, keepdims=True)],
            axis=0,
        )
        for copy in range(part_ref.shape[0]):
            part_ref[copy] = total


def backward_kernel(
    in_ref, mo_ref, carried_ref, stats_ref, gain_ref, skip_ref, out_ref, carry, sums
):
    step_id = pl.program_id(0)

    @pl.when(step_id == 0)
    def _():
        carry[...] = jnp.zeros_like(carry)
        sums[...] = shared_sums(stats_ref)

    gain = gain_ref[...]
    skip = skip_lanes(skip_ref)
    row_id = lax.broadcasted_iota(jnp.int32, (T, T), 0)
    lane_id = lax.broadcasted_iota(jnp.int32, (T, T), 1)
    later = row_id <= lane_id
    state = carry[...]
    results = []
    first = BLOCKS_PER_STEP * (STEPS - 1 - step_id)
    found = sums[...]
    for b in reversed(range(BLOCKS_PER_STEP)):
        x = in_ref[b, :T, :256].astype(F32)
        up = in_ref[b, :T, 256:512].astype(F32)
        write = in_ref[b, :T, 512:640]
        read = in_ref[b, :T, 640:768]
        out = mo_ref[b]
        log_decay, _, block_decay, cols = scalars(in_ref[b, T:, :])
        _, delta = normalise(found, first + b, out, up, gain)
        scaled = (delta * spread(cols, 24)).astype(BF16)
        half = delta.astype(BF16)
        scores = contract(write, read, ((1,), (1,)))
        score_grad = jnp.zeros((T, T), F32)
        mixed = []
        for i in range(HEADS // 2):
            pair = slice(128 * i, 128 * (i + 1))
            mix_grad = contract(two_heads(x[:, pair]), half[:, pair], ((1,), (1,)))
            mixing = []
            for n, j in enumerate((2 * i, 2 * i + 1)):
                gap = jnp.where(later, log_decay[j : j + 1] - cols[:, j : j + 1], FAR)
                weight = jnp.exp(gap) * cols[:, 8 + j : 9 + j]
                mixing.append((scores * weight).astype(BF16))
                score_grad = score_grad + weight * mix_grad[T * n : T * (n + 1)]
            mixed.append(
                contract(
                    jnp.concatenate(mixing, axis=1), two_heads(delta[:, pair]), ((1,), (0,))
                )
            )
        carried_grad = state.astype(BF16)
        mixer_grad = (
            jnp.concatenate(mixed, axis=1)
            + spread(cols, 16) * contract(write, carried_grad, ((1,), (0,)))
            + skip * delta
        )
        read_grad = contract(score_grad.astype(BF16), write, ((0,), (0,))) + contract(
            scaled, carried_ref[b], ((1,), (1,))
        )
        state_grad = contract(read, scaled, ((0,), (0,))).astype(BF16).astype(F32)
        state = (state_grad + spread_rows(block_decay) * state).astype(BF16).astype(F32)
        results.append((b, mixer_grad, read_grad))
    for b, mixer_grad, read_grad in results:
        out_ref[b, :, :256] = mixer_grad.astype(BF16)
        out_ref[b, :, 256:] = read_grad.astype(BF16)
    carry[...] = state


def unpack_kernel(in_ref, mixer_ref, read_ref):
    for g in range(G):
        total = jnp.zeros((T, N), F32)
        for d in range(4 * g, 4 * g + 4):
            mixer_ref[:, LANES * d : LANES * (d + 1)] = in_ref[d, :, :256]
            total = total + in_ref[d, :, 256:].astype(F32)
        read_ref[:, N * g : N * (g + 1)] = total.astype(BF16)


def whole(shape):
    return pl.BlockSpec(shape, lambda i: (0,) * len(shape))


SCALARS = pl.BlockSpec(memory_space=pltpu.SMEM)


def call(kernel, grid, in_specs, out_specs, out_shape, scratch=(), flops=0, interpret=False):
    return pl.pallas_call(
        kernel,
        grid=(grid,),
        in_specs=in_specs,
        out_specs=out_specs,
        out_shape=out_shape,
        scratch_shapes=scratch,
        cost_estimate=pl.CostEstimate(flops=flops, bytes_accessed=1 << 20, transcendentals=0),
        interpret=interpret,
    )


def shape(dims, dtype):
    return jax.ShapeDtypeStruct(dims, dtype)


def build(interpret):
    def mixer(mixer_in, write_proj, read_proj, dt_steps, decay_exp, norm_gain, skip_gain, out_grad):
        def exchange(array, axes):
            return lax.all_to_all(array, axes, split_axis=0, concat_axis=0, tiled=True)

        gain = norm_gain.reshape(1, LANES)
        column = lambda i: (0, i)
        sent = call(
            pack_kernel,
            PACK_STEPS,
            [
                pl.BlockSpec((T, H * P_SIZE // PACK_STEPS), column),
                pl.BlockSpec((T, H * P_SIZE // PACK_STEPS), column),
                pl.BlockSpec((T, G * N // PACK_STEPS), column),
                pl.BlockSpec((T, G * N // PACK_STEPS), column),
                pl.BlockSpec((H // PACK_STEPS, T), lambda i: (i, 0)),
                pl.BlockSpec((H // PACK_STEPS, T), lambda i: (i, 0)),
            ],
            pl.BlockSpec((D // PACK_STEPS, T + 8, 768), lambda i: (i, 0, 0)),
            shape((D, T + 8, 768), BF16),
            interpret=interpret,
        )(
            mixer_in[0],
            out_grad[0],
            write_proj[0],
            read_proj[0],
            jnp.transpose(dt_steps[0]),
            jnp.transpose(decay_exp[0]),
        )
        blocks = exchange(sent, SEQ)

        along = lambda i: (i, 0, 0)
        size = BLOCKS_PER_STEP
        mixer_out, carried, stats = call(
            forward_kernel,
            STEPS,
            [pl.BlockSpec((size, T + 8, 768), along), whole((1, LANES)), SCALARS],
            [
                pl.BlockSpec((size, T, LANES), along),
                pl.BlockSpec((size, N, LANES), along),
                whole((4, 2 * D, T)),
            ],
            [
                shape((D, T, LANES), F32),
                shape((D, N, LANES), BF16),
                shape((4, 2 * D, T), F32),
            ],
            [pltpu.VMEM((N, LANES), F32), pltpu.VMEM((T, T), F32)],
            interpret=interpret,
        )(blocks, gain, skip_gain)
        stats = exchange(stats, "seq_1")

        far = lax.axis_size("z_high")
        copies = call(
            gain_kernel,
            D // GAIN_BLOCKS,
            [
                pl.BlockSpec((GAIN_BLOCKS, T, 512), along),
                pl.BlockSpec((GAIN_BLOCKS, T, LANES), along),
                whole((4, 2 * D, T)),
                whole((1, LANES)),
            ],
            whole((far, 2, LANES)),
            shape((far, 2, LANES), F32),
            [pltpu.VMEM((T, T), F32), pltpu.VMEM((2, 8, LANES), F32)],
            interpret=interpret,
        )(blocks, mixer_out, stats, gain)
        parts = exchange(copies, "z_high") if far > 1 else copies
        back = lambda i: (STEPS - 1 - i, 0, 0)
        grads = call(
            backward_kernel,
            STEPS,
            [
                pl.BlockSpec((size, T + 8, 768), back),
                pl.BlockSpec((size, T, LANES), back),
                pl.BlockSpec((size, N, LANES), back),
                whole((4, 2 * D, T)),
                whole((1, LANES)),
                SCALARS,
            ],
            pl.BlockSpec((size, T, 384), back),
            shape((D, T, 384), BF16),
            [pltpu.VMEM((N, LANES), F32), pltpu.VMEM((T, T), F32)],
            flops=1 << 34,
            interpret=interpret,
        )(blocks, mixer_out, carried, stats, gain, skip_gain)
        grads = exchange(grads, SEQ)
        parts = jnp.sum(parts, axis=0)
        for axis in ("core", "z_low"):
            if lax.axis_size(axis) == 2:
                parts = parts + lax.ppermute(parts, axis, [(0, 1), (1, 0)])
        mixer_grad, read_grad = pl.pallas_call(
            unpack_kernel,
            in_specs=[pl.BlockSpec(memory_space=pltpu.VMEM)],
            out_shape=[shape((T, H * P_SIZE), BF16), shape((T, G * N), BF16)],
            interpret=interpret,
        )(grads)
        return (
            mixer_grad[None],
            read_grad[None],
            parts[0],
            jnp.sum(parts[1].reshape(HEADS, P_SIZE), axis=1),
        )

    return mixer


def sharded(mesh, interpret=False):
    rep = ("z_high", "z_low", "core")
    big = P(rep, SEQ, None)
    return jax.shard_map(
        build(interpret),
        mesh=mesh,
        in_specs=(big, big, big, big, big, P(SEQ), P(SEQ), big),
        out_specs=(big, big, P(SEQ), P(SEQ)),
        check_vma=False,
    )


def solution(mesh):
    names = ("seq_0", "seq_1", "z_high", "z_low", "core")
    step = sharded(Mesh(mesh.devices.reshape(4, 4, 16, 2, 2), names))
    return step
```

```python
import jax
import jax.numpy as jnp
from jax import lax
from jax.experimental import pallas as pl
from jax.experimental.pallas import tpu as pltpu
from jax.sharding import Mesh
from jax.sharding import PartitionSpec as P


H = 64
P_SIZE = 64
N = 128
G = 4
HG = 16
T = 128
D = 16
HEADS = H // D
LANES = HEADS * P_SIZE
SEQ = ("seq_0", "seq_1")
F32 = jnp.float32
BF16 = jnp.bfloat16
BLOCKS_PER_STEP = 4
STEPS = D // BLOCKS_PER_STEP
PACK_STEPS = 2
GAIN_BLOCKS = 8
FAR = -1e30
X_AT, UP_AT, WRITE_AT, READ_AT, TAIL_AT, ROWS = 0, 256, 512, 640, 768, 784


def contract(left, right, dims):
    return lax.dot_general(left, right, (dims, ((), ())), preferred_element_type=F32)


def pack_kernel(x_ref, up_ref, write_ref, read_ref, dt_ref, dec_ref, out_ref):
    dec = dec_ref[...]
    high = (dec >> 8).astype(F32)
    low = (dec & 255).astype(F32)
    steps = dt_ref[...].astype(F32)
    top = lax.broadcasted_iota(jnp.int32, (8, 128), 0) < HEADS
    for j in range(D // PACK_STEPS):
        group = slice(N * (j // 4), N * (j // 4 + 1))
        for half in range(2):
            cols = slice(LANES * j + 128 * half, LANES * j + 128 * (half + 1))
            out_ref[j, X_AT + T * half : X_AT + T * (half + 1)] = x_ref[:, cols]
            out_ref[j, UP_AT + T * half : UP_AT + T * (half + 1)] = up_ref[:, cols]
        out_ref[j, WRITE_AT : WRITE_AT + T] = write_ref[:, group]
        out_ref[j, READ_AT : READ_AT + T] = read_ref[:, group]
        base = 8 * (j // 2)
        steps8, high8, low8 = (rows[base : base + 8] for rows in (steps, high, low))
        if j % 2 == 1:
            steps8, low8 = pltpu.roll(steps8, HEADS, 0), pltpu.roll(low8, HEADS, 0)
        else:
            high8 = pltpu.roll(high8, HEADS, 0)
        tail = jnp.concatenate([jnp.where(top, steps8, high8), low8], axis=0)
        out_ref[j, TAIL_AT:ROWS] = tail.astype(BF16)


def wide(ref, b, at):
    return jnp.concatenate([ref[b, at : at + T], ref[b, at + T : at + 2 * T]], axis=1).astype(F32)


def rows_of(tail):
    upto = (
        lax.broadcasted_iota(jnp.int32, (T, T), 0) <= lax.broadcasted_iota(jnp.int32, (T, T), 1)
    ).astype(F32).astype(BF16)
    tail = tail.astype(F32)
    step = tail[:8] / 16.0
    high = pltpu.roll(tail[:8], HEADS, 0).astype(BF16)
    whole = contract(high, upto, ((1,), (0,))) * 256.0 + contract(
        tail[8:].astype(BF16), upto, ((1,), (0,))
    )
    log_decay = -(whole / 65536.0)
    last = jnp.broadcast_to(log_decay[:, T - 1 : T], (8, T))
    ending = jnp.exp(last - log_decay) * step
    readout = jnp.exp(log_decay)
    block_decay = jnp.exp(last).astype(BF16).astype(F32)
    return log_decay, step, block_decay, ending, readout


def scalars(tail):
    log_decay, step, block_decay, ending, readout = rows_of(tail)
    cols = jnp.transpose(jnp.concatenate([log_decay, step, ending, readout], axis=0))
    return log_decay, step, block_decay, cols


def thirds(rows):
    high = rows.astype(BF16).astype(F32)
    middle = (rows - high).astype(BF16).astype(F32)
    return high, middle, rows - high - middle


def head_marks(rows, width):
    row = lax.broadcasted_iota(jnp.int32, (rows, HEADS * width), 0) % 8
    lane = lax.broadcasted_iota(jnp.int32, (rows, HEADS * width), 1) // width
    return (row == lane).astype(F32)


def gaps(log_decay, marks):
    parts = thirds(log_decay)
    place = lax.broadcasted_iota(jnp.int32, (8, T), 0)
    minus = []
    for j in range(HEADS):
        tile = jnp.zeros((8, T), F32)
        for n, part in enumerate(parts):
            tile = jnp.where(place == n, -part[j : j + 1], tile)
        minus.append(tile)
    left = jnp.concatenate([*parts, jnp.ones((8, T), F32)], axis=0).astype(BF16)
    right = jnp.concatenate([marks, jnp.concatenate(minus, axis=1)], axis=0).astype(BF16)
    return contract(left, right, ((0,), (0,)))


def spread_two(ending, readout, marks):
    both = []
    for rows in (ending, readout):
        left = jnp.concatenate(thirds(rows), axis=0).astype(BF16)
        both.append(contract(left, marks, ((0,), (0,))))
    return both


def low_half(shape):
    return lax.broadcasted_iota(jnp.int32, shape, len(shape) - 1) < P_SIZE


def spread(cols, at):
    mask = low_half((T, 128))
    pairs = []
    for i in range(HEADS // 2):
        a = jnp.broadcast_to(cols[:, at + 2 * i : at + 2 * i + 1], (T, 128))
        b = jnp.broadcast_to(cols[:, at + 2 * i + 1 : at + 2 * i + 2], (T, 128))
        pairs.append(jnp.where(mask, a, b))
    return jnp.concatenate(pairs, axis=1)


def spread_rows(rows):
    mask = low_half((1, 128))
    return jnp.concatenate(
        [
            jnp.where(mask, rows[2 * i : 2 * i + 1], rows[2 * i + 1 : 2 * i + 2])
            for i in range(HEADS // 2)
        ],
        axis=1,
    )


def skip_lanes(skip_ref):
    lane = lax.broadcasted_iota(jnp.int32, (1, LANES), 1) // P_SIZE
    row = jnp.full((1, LANES), skip_ref[HEADS - 1], F32)
    for j in range(HEADS - 1):
        row = jnp.where(lane == j, skip_ref[j], row)
    return row


def two_heads(pair):
    mask = low_half((T, 128))
    return jnp.concatenate(
        [jnp.where(mask, pair, 0.0).astype(BF16), jnp.where(mask, 0.0, pair).astype(BF16)], axis=0
    )


def forward_kernel(in_ref, gain_ref, skip_ref, mo_ref, carried_ref, stats_ref, carry, sums):
    step_id = pl.program_id(0)

    @pl.when(step_id == 0)
    def _():
        carry[...] = jnp.zeros_like(carry)
        sums[...] = jnp.zeros_like(sums)

    gain = gain_ref[...]
    skip = skip_lanes(skip_ref)
    row_id = lax.broadcasted_iota(jnp.int32, (T, T), 0)
    lane_id = lax.broadcasted_iota(jnp.int32, (T, T), 1)
    causal = row_id >= lane_id
    marks = head_marks(24, P_SIZE).astype(BF16)
    wide_marks = head_marks(24, T)
    state = carry[...]
    found = sums[...]
    results = []
    for b in range(BLOCKS_PER_STEP):
        x = wide(in_ref, b, X_AT)
        up = wide(in_ref, b, UP_AT)
        write = in_ref[b, WRITE_AT : WRITE_AT + T]
        read = in_ref[b, READ_AT : READ_AT + T]
        log_decay, step, block_decay, ending, readout = rows_of(in_ref[b, TAIL_AT:])
        gap = gaps(log_decay, wide_marks)
        ending, readout = spread_two(ending, readout, marks)
        scores = contract(read, write, ((1,), (1,)))
        inner = []
        for i in range(HEADS // 2):
            mixing = []
            for j in (2 * i, 2 * i + 1):
                decay = jnp.exp(jnp.where(causal, gap[:, T * j : T * (j + 1)], FAR))
                mixing.append((scores * (decay * step[j : j + 1])).astype(BF16))
            inner.append(
                contract(
                    jnp.concatenate(mixing, axis=1),
                    two_heads(x[:, 128 * i : 128 * (i + 1)]),
                    ((1,), (0,)),
                )
            )
        weighted = (x * ending).astype(BF16)
        span_state = contract(write, weighted, ((0,), (0,))).astype(BF16).astype(F32)
        carried = state.astype(BF16)
        state = (spread_rows(block_decay) * state + span_state).astype(BF16).astype(F32)
        out = (
            jnp.concatenate(inner, axis=1)
            + readout * contract(read, carried, ((1,), (0,)))
            + skip * x
        )
        square = jnp.sum(out * out, axis=1, keepdims=True)
        cross = jnp.sum(up * gain * out, axis=1, keepdims=True)
        at = BLOCKS_PER_STEP * step_id + b
        found = jnp.where(lane_id == at, square, jnp.where(lane_id == D + at, cross, found))
        results.append((out, carried))
    for b, (out, carried) in enumerate(results):
        mo_ref[b] = out
        carried_ref[b] = carried
    carry[...] = state
    sums[...] = found

    @pl.when(step_id == STEPS - 1)
    def _():
        rows = jnp.transpose(sums[...])[: 2 * D]
        for d in range(4):
            stats_ref[d] = rows


def shared_sums(stats_ref, sums):
    total = stats_ref[0] + stats_ref[1] + stats_ref[2] + stats_ref[3]
    inverse = lax.rsqrt(total[:D] / (HG * P_SIZE) + 1e-05)
    mean = inverse * total[D:] / (HG * P_SIZE)
    for n, part in enumerate((*thirds(inverse), *thirds(mean))):
        sums[n] = part


def normalise(sums, block, out, up, gain):
    place = lax.broadcasted_iota(jnp.int32, (8, T), 0)
    rows = jnp.zeros((8, T), F32)
    for n in range(6):
        rows = jnp.where(place == n, sums[n, pl.ds(block, 1), :], rows)
    row = lax.broadcasted_iota(jnp.int32, (8, 2 * LANES), 0) // 3
    lane = lax.broadcasted_iota(jnp.int32, (8, 2 * LANES), 1) // LANES
    both = contract(rows.astype(BF16), (row == lane).astype(F32).astype(BF16), ((0,), (0,)))
    inverse, mean = both[:, :LANES], both[:, LANES:]
    normed = out * inverse
    return normed, inverse * (up * gain - normed * mean)


def gain_kernel(in_ref, mo_ref, stats_ref, gain_ref, part_ref, sums, parts):
    step_id = pl.program_id(0)

    @pl.when(step_id == 0)
    def _():
        parts[...] = jnp.zeros_like(parts)
        shared_sums(stats_ref, sums)

    gain = gain_ref[...]
    gain_sum = parts[0]
    skip_sum = parts[1]
    for b in range(GAIN_BLOCKS):
        x = wide(in_ref, b, X_AT)
        up = wide(in_ref, b, UP_AT)
        normed, delta = normalise(sums, GAIN_BLOCKS * step_id + b, mo_ref[b], up, gain)
        gain_sum = gain_sum + jnp.sum((up * normed).reshape(T // 8, 8, LANES), axis=0)
        skip_sum = skip_sum + jnp.sum((delta * x).reshape(T // 8, 8, LANES), axis=0)
    parts[0] = gain_sum
    parts[1] = skip_sum

    @pl.when(step_id == D // GAIN_BLOCKS - 1)
    def _():
        total = jnp.concatenate(
            [jnp.sum(parts[0], axis=0, keepdims=True), jnp.sum(parts[1], axis=0, keepdims=True)],
            axis=0,
        )
        for copy in range(part_ref.shape[0]):
            part_ref[copy] = total


def backward_kernel(
    in_ref, mo_ref, carried_ref, stats_ref, gain_ref, skip_ref, out_ref, carry, sums
):
    step_id = pl.program_id(0)

    @pl.when(step_id == 0)
    def _():
        carry[...] = jnp.zeros_like(carry)
        shared_sums(stats_ref, sums)

    gain = gain_ref[...]
    skip = skip_lanes(skip_ref)
    row_id = lax.broadcasted_iota(jnp.int32, (T, T), 0)
    lane_id = lax.broadcasted_iota(jnp.int32, (T, T), 1)
    later = row_id <= lane_id
    state = carry[...]
    results = []
    first = BLOCKS_PER_STEP * (STEPS - 1 - step_id)
    for b in reversed(range(BLOCKS_PER_STEP)):
        x = wide(in_ref, b, X_AT)
        up = wide(in_ref, b, UP_AT)
        write = in_ref[b, WRITE_AT : WRITE_AT + T]
        read = in_ref[b, READ_AT : READ_AT + T]
        out = mo_ref[b]
        log_decay, _, block_decay, cols = scalars(in_ref[b, TAIL_AT:])
        _, delta = normalise(sums, first + b, out, up, gain)
        scaled = (delta * spread(cols, 24)).astype(BF16)
        half = delta.astype(BF16)
        scores = contract(write, read, ((1,), (1,)))
        score_grad = jnp.zeros((T, T), F32)
        mixed = []
        for i in range(HEADS // 2):
            pair = slice(128 * i, 128 * (i + 1))
            mix_grad = contract(two_heads(x[:, pair]), half[:, pair], ((1,), (1,)))
            mixing = []
            for n, j in enumerate((2 * i, 2 * i + 1)):
                gap = jnp.where(later, log_decay[j : j + 1] - cols[:, j : j + 1], FAR)
                weight = jnp.exp(gap) * cols[:, 8 + j : 9 + j]
                mixing.append((scores * weight).astype(BF16))
                score_grad = score_grad + weight * mix_grad[T * n : T * (n + 1)]
            mixed.append(
                contract(
                    jnp.concatenate(mixing, axis=1), two_heads(delta[:, pair]), ((1,), (0,))
                )
            )
        carried_grad = state.astype(BF16)
        mixer_grad = (
            jnp.concatenate(mixed, axis=1)
            + spread(cols, 16) * contract(write, carried_grad, ((1,), (0,)))
            + skip * delta
        )
        read_grad = contract(score_grad.astype(BF16), write, ((0,), (0,))) + contract(
            scaled, carried_ref[b], ((1,), (1,))
        )
        state_grad = contract(read, scaled, ((0,), (0,))).astype(BF16).astype(F32)
        state = (state_grad + spread_rows(block_decay) * state).astype(BF16).astype(F32)
        results.append((b, mixer_grad, read_grad))
    for b, mixer_grad, read_grad in results:
        mixer_grad = mixer_grad.astype(BF16)
        out_ref[b, :T] = mixer_grad[:, :128]
        out_ref[b, T : 2 * T] = mixer_grad[:, 128:]
        out_ref[b, 2 * T :] = read_grad.astype(BF16)
    carry[...] = state


def unpack_kernel(in_ref, mixer_ref, read_ref):
    for g in range(G):
        total = jnp.zeros((T, N), F32)
        for d in range(4 * g, 4 * g + 4):
            for half in range(2):
                at = LANES * d + 128 * half
                mixer_ref[:, at : at + 128] = in_ref[d, T * half : T * (half + 1)]
            total = total + in_ref[d, 2 * T :].astype(F32)
        read_ref[:, N * g : N * (g + 1)] = total.astype(BF16)


def whole(shape):
    return pl.BlockSpec(shape, lambda i: (0,) * len(shape))


SCALARS = pl.BlockSpec(memory_space=pltpu.SMEM)


def call(kernel, grid, in_specs, out_specs, out_shape, scratch=(), flops=0, interpret=False):
    return pl.pallas_call(
        kernel,
        grid=(grid,),
        in_specs=in_specs,
        out_specs=out_specs,
        out_shape=out_shape,
        scratch_shapes=scratch,
        cost_estimate=pl.CostEstimate(flops=flops, bytes_accessed=1 << 20, transcendentals=0),
        interpret=interpret,
    )


def shape(dims, dtype):
    return jax.ShapeDtypeStruct(dims, dtype)


def build(interpret):
    def mixer(mixer_in, write_proj, read_proj, dt_steps, decay_exp, norm_gain, skip_gain, out_grad):
        def exchange(array, axes):
            return lax.all_to_all(array, axes, split_axis=0, concat_axis=0, tiled=True)

        gain = norm_gain.reshape(1, LANES)
        column = lambda i: (0, i)
        sent = call(
            pack_kernel,
            PACK_STEPS,
            [
                pl.BlockSpec((T, H * P_SIZE // PACK_STEPS), column),
                pl.BlockSpec((T, H * P_SIZE // PACK_STEPS), column),
                pl.BlockSpec((T, G * N // PACK_STEPS), column),
                pl.BlockSpec((T, G * N // PACK_STEPS), column),
                pl.BlockSpec((H // PACK_STEPS, T), lambda i: (i, 0)),
                pl.BlockSpec((H // PACK_STEPS, T), lambda i: (i, 0)),
            ],
            pl.BlockSpec((D // PACK_STEPS, ROWS, 128), lambda i: (i, 0, 0)),
            shape((D, ROWS, 128), BF16),
            interpret=interpret,
        )(
            mixer_in[0],
            out_grad[0],
            write_proj[0],
            read_proj[0],
            jnp.transpose(dt_steps[0]),
            jnp.transpose(decay_exp[0]),
        )
        blocks = exchange(sent, SEQ)

        along = lambda i: (i, 0, 0)
        size = BLOCKS_PER_STEP
        mixer_out, carried, stats = call(
            forward_kernel,
            STEPS,
            [pl.BlockSpec((size, ROWS, 128), along), whole((1, LANES)), SCALARS],
            [
                pl.BlockSpec((size, T, LANES), along),
                pl.BlockSpec((size, N, LANES), along),
                whole((4, 2 * D, T)),
            ],
            [
                shape((D, T, LANES), F32),
                shape((D, N, LANES), BF16),
                shape((4, 2 * D, T), F32),
            ],
            [pltpu.VMEM((N, LANES), F32), pltpu.VMEM((T, T), F32)],
            interpret=interpret,
        )(blocks, gain, skip_gain)
        stats = exchange(stats, "seq_1")

        far = lax.axis_size("z_high")
        copies = call(
            gain_kernel,
            D // GAIN_BLOCKS,
            [
                pl.BlockSpec((GAIN_BLOCKS, WRITE_AT, 128), along),
                pl.BlockSpec((GAIN_BLOCKS, T, LANES), along),
                whole((4, 2 * D, T)),
                whole((1, LANES)),
            ],
            whole((far, 2, LANES)),
            shape((far, 2, LANES), F32),
            [pltpu.VMEM((6, D, T), F32), pltpu.VMEM((2, 8, LANES), F32)],
            interpret=interpret,
        )(blocks, mixer_out, stats, gain)
        parts = exchange(copies, "z_high") if far > 1 else copies
        back = lambda i: (STEPS - 1 - i, 0, 0)
        grads = call(
            backward_kernel,
            STEPS,
            [
                pl.BlockSpec((size, ROWS, 128), back),
                pl.BlockSpec((size, T, LANES), back),
                pl.BlockSpec((size, N, LANES), back),
                whole((4, 2 * D, T)),
                whole((1, LANES)),
                SCALARS,
            ],
            pl.BlockSpec((size, 3 * T, 128), back),
            shape((D, 3 * T, 128), BF16),
            [pltpu.VMEM((N, LANES), F32), pltpu.VMEM((6, D, T), F32)],
            flops=1 << 34,
            interpret=interpret,
        )(blocks, mixer_out, carried, stats, gain, skip_gain)
        grads = exchange(grads, SEQ)
        parts = jnp.sum(parts, axis=0)
        for axis in ("core", "z_low"):
            if lax.axis_size(axis) == 2:
                parts = parts + lax.ppermute(parts, axis, [(0, 1), (1, 0)])
        mixer_grad, read_grad = pl.pallas_call(
            unpack_kernel,
            out_shape=[shape((T, H * P_SIZE), BF16), shape((T, G * N), BF16)],
            interpret=interpret,
        )(grads)
        return (
            mixer_grad[None],
            read_grad[None],
            parts[0],
            jnp.sum(parts[1].reshape(HEADS, P_SIZE), axis=1),
        )

    return mixer


def sharded(mesh, interpret=False):
    rep = ("z_high", "z_low", "core")
    big = P(rep, SEQ, None)
    return jax.shard_map(
        build(interpret),
        mesh=mesh,
        in_specs=(big, big, big, big, big, P(SEQ), P(SEQ), big),
        out_specs=(big, big, P(SEQ), P(SEQ)),
        check_vma=False,
    )


def solution(mesh):
    names = ("seq_0", "seq_1", "z_high", "z_low", "core")
    step = sharded(Mesh(mesh.devices.reshape(4, 4, 16, 2, 2), names))
    return step
```

```python
import jax
import jax.numpy as jnp
from jax import lax
from jax.experimental import pallas as pl
from jax.experimental.pallas import tpu as pltpu
from jax.sharding import Mesh
from jax.sharding import PartitionSpec as P


H = 64
P_SIZE = 64
N = 128
G = 4
HG = 16
T = 128
D = 16
HEADS = H // D
LANES = HEADS * P_SIZE
SEQ = ("seq_0", "seq_1")
NEAR = ("z_low", "core")
F32 = jnp.float32
BF16 = jnp.bfloat16
BLOCKS_PER_STEP = 4
STEPS = D // BLOCKS_PER_STEP
PACK_STEPS = 2
GAIN_BLOCKS = 8
FAR = -1e30
X_AT, UP_AT, WRITE_AT, READ_AT, TAIL_AT, ROWS = 0, 256, 512, 640, 768, 784


def contract(left, right, dims):
    return lax.dot_general(left, right, (dims, ((), ())), preferred_element_type=F32)


def pack_kernel(x_ref, up_ref, write_ref, read_ref, dt_ref, dec_ref, out_ref):
    dec = dec_ref[...]
    high = (dec >> 8).astype(F32)
    low = (dec & 255).astype(F32)
    steps = dt_ref[...].astype(F32)
    top = lax.broadcasted_iota(jnp.int32, (8, 128), 0) < HEADS
    for j in range(D // PACK_STEPS):
        group = slice(N * (j // 4), N * (j // 4 + 1))
        for half in range(2):
            cols = slice(LANES * j + 128 * half, LANES * j + 128 * (half + 1))
            out_ref[j, X_AT + T * half : X_AT + T * (half + 1)] = x_ref[:, cols]
            out_ref[j, UP_AT + T * half : UP_AT + T * (half + 1)] = up_ref[:, cols]
        out_ref[j, WRITE_AT : WRITE_AT + T] = write_ref[:, group]
        out_ref[j, READ_AT : READ_AT + T] = read_ref[:, group]
        base = 8 * (j // 2)
        steps8, high8, low8 = (rows[base : base + 8] for rows in (steps, high, low))
        if j % 2 == 1:
            steps8, low8 = pltpu.roll(steps8, HEADS, 0), pltpu.roll(low8, HEADS, 0)
        else:
            high8 = pltpu.roll(high8, HEADS, 0)
        tail = jnp.concatenate([jnp.where(top, steps8, high8), low8], axis=0)
        out_ref[j, TAIL_AT:ROWS] = tail.astype(BF16)


def wide(ref, b, at):
    return jnp.concatenate([ref[b, at : at + T], ref[b, at + T : at + 2 * T]], axis=1).astype(F32)


def rows_of(tail):
    upto = (
        lax.broadcasted_iota(jnp.int32, (T, T), 0) <= lax.broadcasted_iota(jnp.int32, (T, T), 1)
    ).astype(F32).astype(BF16)
    tail = tail.astype(F32)
    step = tail[:8] / 16.0
    high = pltpu.roll(tail[:8], HEADS, 0).astype(BF16)
    whole = contract(high, upto, ((1,), (0,))) * 256.0 + contract(
        tail[8:].astype(BF16), upto, ((1,), (0,))
    )
    log_decay = -(whole / 65536.0)
    last = jnp.broadcast_to(log_decay[:, T - 1 : T], (8, T))
    ending = jnp.exp(last - log_decay) * step
    readout = jnp.exp(log_decay)
    block_decay = jnp.exp(last).astype(BF16).astype(F32)
    return log_decay, step, block_decay, ending, readout


def scalars(tail):
    log_decay, step, block_decay, ending, readout = rows_of(tail)
    cols = jnp.transpose(jnp.concatenate([log_decay, step, ending, readout], axis=0))
    return log_decay, step, block_decay, cols


def thirds(rows):
    high = rows.astype(BF16).astype(F32)
    middle = (rows - high).astype(BF16).astype(F32)
    return high, middle, rows - high - middle


def head_marks(rows, width):
    row = lax.broadcasted_iota(jnp.int32, (rows, HEADS * width), 0) % 8
    lane = lax.broadcasted_iota(jnp.int32, (rows, HEADS * width), 1) // width
    return (row == lane).astype(F32)


def gaps(log_decay, marks):
    parts = thirds(log_decay)
    place = lax.broadcasted_iota(jnp.int32, (8, T), 0)
    minus = []
    for j in range(HEADS):
        tile = jnp.zeros((8, T), F32)
        for n, part in enumerate(parts):
            tile = jnp.where(place == n, -part[j : j + 1], tile)
        minus.append(tile)
    left = jnp.concatenate([*parts, jnp.ones((8, T), F32)], axis=0).astype(BF16)
    right = jnp.concatenate([marks, jnp.concatenate(minus, axis=1)], axis=0).astype(BF16)
    return contract(left, right, ((0,), (0,)))


def spread_two(ending, readout, marks):
    both = []
    for rows in (ending, readout):
        left = jnp.concatenate(thirds(rows), axis=0).astype(BF16)
        both.append(contract(left, marks, ((0,), (0,))))
    return both


def low_half(shape):
    return lax.broadcasted_iota(jnp.int32, shape, len(shape) - 1) < P_SIZE


def spread(cols, at):
    mask = low_half((T, 128))
    pairs = []
    for i in range(HEADS // 2):
        a = jnp.broadcast_to(cols[:, at + 2 * i : at + 2 * i + 1], (T, 128))
        b = jnp.broadcast_to(cols[:, at + 2 * i + 1 : at + 2 * i + 2], (T, 128))
        pairs.append(jnp.where(mask, a, b))
    return jnp.concatenate(pairs, axis=1)


def spread_rows(rows):
    mask = low_half((1, 128))
    return jnp.concatenate(
        [
            jnp.where(mask, rows[2 * i : 2 * i + 1], rows[2 * i + 1 : 2 * i + 2])
            for i in range(HEADS // 2)
        ],
        axis=1,
    )


def skip_lanes(skip_ref):
    lane = lax.broadcasted_iota(jnp.int32, (1, LANES), 1) // P_SIZE
    row = jnp.full((1, LANES), skip_ref[HEADS - 1], F32)
    for j in range(HEADS - 1):
        row = jnp.where(lane == j, skip_ref[j], row)
    return row


def two_heads(pair):
    mask = low_half((T, 128))
    return jnp.concatenate(
        [jnp.where(mask, pair, 0.0).astype(BF16), jnp.where(mask, 0.0, pair).astype(BF16)], axis=0
    )


def forward_kernel(in_ref, gain_ref, skip_ref, mo_ref, carried_ref, stats_ref, carry, sums):
    step_id = pl.program_id(0)

    @pl.when(step_id == 0)
    def _():
        carry[...] = jnp.zeros_like(carry)
        sums[...] = jnp.zeros_like(sums)

    gain = gain_ref[...]
    skip = skip_lanes(skip_ref)
    row_id = lax.broadcasted_iota(jnp.int32, (T, T), 0)
    lane_id = lax.broadcasted_iota(jnp.int32, (T, T), 1)
    causal = row_id >= lane_id
    marks = head_marks(24, P_SIZE).astype(BF16)
    wide_marks = head_marks(24, T)
    state = carry[...]
    found = sums[...]
    results = []
    for b in range(BLOCKS_PER_STEP):
        x = wide(in_ref, b, X_AT)
        up = wide(in_ref, b, UP_AT)
        write = in_ref[b, WRITE_AT : WRITE_AT + T]
        read = in_ref[b, READ_AT : READ_AT + T]
        log_decay, step, block_decay, ending, readout = rows_of(in_ref[b, TAIL_AT:])
        gap = gaps(log_decay, wide_marks)
        ending, readout = spread_two(ending, readout, marks)
        scores = contract(read, write, ((1,), (1,)))
        inner = []
        for i in range(HEADS // 2):
            mixing = []
            for j in (2 * i, 2 * i + 1):
                decay = jnp.exp(jnp.where(causal, gap[:, T * j : T * (j + 1)], FAR))
                mixing.append((scores * (decay * step[j : j + 1])).astype(BF16))
            inner.append(
                contract(
                    jnp.concatenate(mixing, axis=1),
                    two_heads(x[:, 128 * i : 128 * (i + 1)]),
                    ((1,), (0,)),
                )
            )
        weighted = (x * ending).astype(BF16)
        span_state = contract(write, weighted, ((0,), (0,))).astype(BF16).astype(F32)
        carried = state.astype(BF16)
        state = (spread_rows(block_decay) * state + span_state).astype(BF16).astype(F32)
        out = (
            jnp.concatenate(inner, axis=1)
            + readout * contract(read, carried, ((1,), (0,)))
            + skip * x
        )
        square = jnp.sum(out * out, axis=1, keepdims=True)
        cross = jnp.sum(up * gain * out, axis=1, keepdims=True)
        at = BLOCKS_PER_STEP * step_id + b
        found = jnp.where(lane_id == at, square, jnp.where(lane_id == D + at, cross, found))
        results.append((out, carried))
    for b, (out, carried) in enumerate(results):
        mo_ref[b] = out
        carried_ref[b] = carried
    carry[...] = state
    sums[...] = found

    @pl.when(step_id == STEPS - 1)
    def _():
        rows = jnp.transpose(sums[...])[: 2 * D]
        for d in range(4):
            stats_ref[d] = rows


def shared_sums(stats_ref, sums):
    total = stats_ref[0] + stats_ref[1] + stats_ref[2] + stats_ref[3]
    inverse = lax.rsqrt(total[:D] / (HG * P_SIZE) + 1e-05)
    mean = inverse * total[D:] / (HG * P_SIZE)
    for n, part in enumerate((*thirds(inverse), *thirds(mean))):
        sums[n] = part


def normalise(sums, block, out, up, gain):
    place = lax.broadcasted_iota(jnp.int32, (8, T), 0)
    rows = jnp.zeros((8, T), F32)
    for n in range(6):
        rows = jnp.where(place == n, sums[n, pl.ds(block, 1), :], rows)
    row = lax.broadcasted_iota(jnp.int32, (8, 2 * LANES), 0) // 3
    lane = lax.broadcasted_iota(jnp.int32, (8, 2 * LANES), 1) // LANES
    both = contract(rows.astype(BF16), (row == lane).astype(F32).astype(BF16), ((0,), (0,)))
    inverse, mean = both[:, :LANES], both[:, LANES:]
    normed = out * inverse
    return normed, inverse * (up * gain - normed * mean)


def gain_kernel(in_ref, mo_ref, stats_ref, gain_ref, part_ref, sums, parts):
    step_id = pl.program_id(0)

    @pl.when(step_id == 0)
    def _():
        parts[...] = jnp.zeros_like(parts)
        shared_sums(stats_ref, sums)

    gain = gain_ref[...]
    gain_sum = parts[0]
    skip_sum = parts[1]
    for b in range(GAIN_BLOCKS):
        x = wide(in_ref, b, X_AT)
        up = wide(in_ref, b, UP_AT)
        normed, delta = normalise(sums, GAIN_BLOCKS * step_id + b, mo_ref[b], up, gain)
        gain_sum = gain_sum + jnp.sum((up * normed).reshape(T // 8, 8, LANES), axis=0)
        skip_sum = skip_sum + jnp.sum((delta * x).reshape(T // 8, 8, LANES), axis=0)
    parts[0] = gain_sum
    parts[1] = skip_sum

    @pl.when(step_id == D // GAIN_BLOCKS - 1)
    def _():
        total = jnp.concatenate(
            [jnp.sum(parts[0], axis=0, keepdims=True), jnp.sum(parts[1], axis=0, keepdims=True)],
            axis=0,
        )
        for copy in range(part_ref.shape[0]):
            part_ref[copy] = total


def backward_kernel(
    in_ref, mo_ref, carried_ref, stats_ref, gain_ref, skip_ref, out_ref, carry, sums
):
    step_id = pl.program_id(0)

    @pl.when(step_id == 0)
    def _():
        carry[...] = jnp.zeros_like(carry)
        shared_sums(stats_ref, sums)

    gain = gain_ref[...]
    skip = skip_lanes(skip_ref)
    row_id = lax.broadcasted_iota(jnp.int32, (T, T), 0)
    lane_id = lax.broadcasted_iota(jnp.int32, (T, T), 1)
    later = row_id <= lane_id
    state = carry[...]
    results = []
    first = BLOCKS_PER_STEP * (STEPS - 1 - step_id)
    for b in reversed(range(BLOCKS_PER_STEP)):
        x = wide(in_ref, b, X_AT)
        up = wide(in_ref, b, UP_AT)
        write = in_ref[b, WRITE_AT : WRITE_AT + T]
        read = in_ref[b, READ_AT : READ_AT + T]
        out = mo_ref[b]
        log_decay, _, block_decay, cols = scalars(in_ref[b, TAIL_AT:])
        _, delta = normalise(sums, first + b, out, up, gain)
        scaled = (delta * spread(cols, 24)).astype(BF16)
        half = delta.astype(BF16)
        scores = contract(write, read, ((1,), (1,)))
        score_grad = jnp.zeros((T, T), F32)
        mixed = []
        for i in range(HEADS // 2):
            pair = slice(128 * i, 128 * (i + 1))
            mix_grad = contract(two_heads(x[:, pair]), half[:, pair], ((1,), (1,)))
            mixing = []
            for n, j in enumerate((2 * i, 2 * i + 1)):
                gap = jnp.where(later, log_decay[j : j + 1] - cols[:, j : j + 1], FAR)
                weight = jnp.exp(gap) * cols[:, 8 + j : 9 + j]
                mixing.append((scores * weight).astype(BF16))
                score_grad = score_grad + weight * mix_grad[T * n : T * (n + 1)]
            mixed.append(
                contract(
                    jnp.concatenate(mixing, axis=1), two_heads(delta[:, pair]), ((1,), (0,))
                )
            )
        carried_grad = state.astype(BF16)
        mixer_grad = (
            jnp.concatenate(mixed, axis=1)
            + spread(cols, 16) * contract(write, carried_grad, ((1,), (0,)))
            + skip * delta
        )
        read_grad = contract(score_grad.astype(BF16), write, ((0,), (0,))) + contract(
            scaled, carried_ref[b], ((1,), (1,))
        )
        state_grad = contract(read, scaled, ((0,), (0,))).astype(BF16).astype(F32)
        state = (state_grad + spread_rows(block_decay) * state).astype(BF16).astype(F32)
        results.append((b, mixer_grad, read_grad))
    for b, mixer_grad, read_grad in results:
        mixer_grad = mixer_grad.astype(BF16)
        out_ref[b, :T] = mixer_grad[:, :128]
        out_ref[b, T : 2 * T] = mixer_grad[:, 128:]
        out_ref[b, 2 * T :] = read_grad.astype(BF16)
    carry[...] = state


def unpack_kernel(in_ref, mixer_ref, read_ref):
    for g in range(G):
        total = jnp.zeros((T, N), F32)
        for d in range(4 * g, 4 * g + 4):
            for half in range(2):
                at = LANES * d + 128 * half
                mixer_ref[:, at : at + 128] = in_ref[d, T * half : T * (half + 1)]
            total = total + in_ref[d, 2 * T :].astype(F32)
        read_ref[:, N * g : N * (g + 1)] = total.astype(BF16)


def whole(shape):
    return pl.BlockSpec(shape, lambda i: (0,) * len(shape))


SCALARS = pl.BlockSpec(memory_space=pltpu.SMEM)


def call(kernel, grid, in_specs, out_specs, out_shape, scratch=(), flops=0, interpret=False):
    return pl.pallas_call(
        kernel,
        grid=(grid,),
        in_specs=in_specs,
        out_specs=out_specs,
        out_shape=out_shape,
        scratch_shapes=scratch,
        cost_estimate=pl.CostEstimate(flops=flops, bytes_accessed=1 << 20, transcendentals=0),
        interpret=interpret,
    )


def shape(dims, dtype):
    return jax.ShapeDtypeStruct(dims, dtype)


def build(interpret):
    def mixer(mixer_in, write_proj, read_proj, dt_steps, decay_exp, norm_gain, skip_gain, out_grad):
        def exchange(array, axes):
            return lax.all_to_all(array, axes, split_axis=0, concat_axis=0, tiled=True)

        gain = norm_gain.reshape(1, LANES)
        column = lambda i: (0, i)
        sent = call(
            pack_kernel,
            PACK_STEPS,
            [
                pl.BlockSpec((T, H * P_SIZE // PACK_STEPS), column),
                pl.BlockSpec((T, H * P_SIZE // PACK_STEPS), column),
                pl.BlockSpec((T, G * N // PACK_STEPS), column),
                pl.BlockSpec((T, G * N // PACK_STEPS), column),
                pl.BlockSpec((H // PACK_STEPS, T), lambda i: (i, 0)),
                pl.BlockSpec((H // PACK_STEPS, T), lambda i: (i, 0)),
            ],
            pl.BlockSpec((D // PACK_STEPS, ROWS, 128), lambda i: (i, 0, 0)),
            shape((D, ROWS, 128), BF16),
            interpret=interpret,
        )(
            mixer_in[0],
            out_grad[0],
            write_proj[0],
            read_proj[0],
            jnp.transpose(dt_steps[0]),
            jnp.transpose(decay_exp[0]),
        )
        blocks = exchange(sent, SEQ)

        along = lambda i: (i, 0, 0)
        size = BLOCKS_PER_STEP
        mixer_out, carried, stats = call(
            forward_kernel,
            STEPS,
            [pl.BlockSpec((size, ROWS, 128), along), whole((1, LANES)), SCALARS],
            [
                pl.BlockSpec((size, T, LANES), along),
                pl.BlockSpec((size, N, LANES), along),
                whole((4, 2 * D, T)),
            ],
            [
                shape((D, T, LANES), F32),
                shape((D, N, LANES), BF16),
                shape((4, 2 * D, T), F32),
            ],
            [pltpu.VMEM((N, LANES), F32), pltpu.VMEM((T, T), F32)],
            interpret=interpret,
        )(blocks, gain, skip_gain)
        stats = exchange(stats, "seq_1")

        near = lax.axis_size(NEAR)
        copies = call(
            gain_kernel,
            D // GAIN_BLOCKS,
            [
                pl.BlockSpec((GAIN_BLOCKS, WRITE_AT, 128), along),
                pl.BlockSpec((GAIN_BLOCKS, T, LANES), along),
                whole((4, 2 * D, T)),
                whole((1, LANES)),
            ],
            whole((near, 2, LANES)),
            shape((near, 2, LANES), F32),
            [pltpu.VMEM((6, D, T), F32), pltpu.VMEM((2, 8, LANES), F32)],
            interpret=interpret,
        )(blocks, mixer_out, stats, gain)
        parts = exchange(copies, NEAR) if near > 1 else copies
        back = lambda i: (STEPS - 1 - i, 0, 0)
        grads = call(
            backward_kernel,
            STEPS,
            [
                pl.BlockSpec((size, ROWS, 128), back),
                pl.BlockSpec((size, T, LANES), back),
                pl.BlockSpec((size, N, LANES), back),
                whole((4, 2 * D, T)),
                whole((1, LANES)),
                SCALARS,
            ],
            pl.BlockSpec((size, 3 * T, 128), back),
            shape((D, 3 * T, 128), BF16),
            [pltpu.VMEM((N, LANES), F32), pltpu.VMEM((6, D, T), F32)],
            flops=1 << 34,
            interpret=interpret,
        )(blocks, mixer_out, carried, stats, gain, skip_gain)
        grads = exchange(grads, SEQ)
        parts = jnp.sum(parts, axis=0)
        if lax.axis_size("z_high") == 4:
            one, two, three = (
                lax.ppermute(parts, "z_high", [(i, i ^ d) for i in range(4)]) for d in (1, 2, 3)
            )
            parts = (parts + one) + (two + three)
        mixer_grad, read_grad = pl.pallas_call(
            unpack_kernel,
            out_shape=[shape((T, H * P_SIZE), BF16), shape((T, G * N), BF16)],
            interpret=interpret,
        )(grads)
        return (
            mixer_grad[None],
            read_grad[None],
            parts[0],
            jnp.sum(parts[1].reshape(HEADS, P_SIZE), axis=1),
        )

    return mixer


def sharded(mesh, interpret=False):
    rep = ("z_high", "z_low", "core")
    big = P(rep, SEQ, None)
    return jax.shard_map(
        build(interpret),
        mesh=mesh,
        in_specs=(big, big, big, big, big, P(SEQ), P(SEQ), big),
        out_specs=(big, big, P(SEQ), P(SEQ)),
        check_vma=False,
    )


def solution(mesh):
    names = ("seq_0", "seq_1", "z_high", "z_low", "core")
    step = sharded(Mesh(mesh.devices.reshape(4, 4, 4, 8, 2), names))
    return step
```

```python
import jax
import jax.numpy as jnp
from jax import lax
from jax.experimental import pallas as pl
from jax.experimental.pallas import tpu as pltpu
from jax.sharding import Mesh
from jax.sharding import PartitionSpec as P


H = 64
P_SIZE = 64
N = 128
G = 4
HG = 16
T = 128
D = 16
HEADS = H // D
LANES = HEADS * P_SIZE
SEQ = ("seq_0", "seq_1")
NEAR = ("z_low", "core")
F32 = jnp.float32
BF16 = jnp.bfloat16
BLOCKS_PER_STEP = 4
STEPS = D // BLOCKS_PER_STEP
PACK_STEPS = 2
GAIN_BLOCKS = 8
FAR = -1e30
HELD = 11
X_AT, UP_AT, WRITE_AT, READ_AT, TAIL_AT, ROWS = 0, 256, 512, 640, 768, 784


def contract(left, right, dims):
    return lax.dot_general(left, right, (dims, ((), ())), preferred_element_type=F32)


def pack_kernel(x_ref, up_ref, write_ref, read_ref, dt_ref, dec_ref, out_ref):
    dec = dec_ref[...]
    high = (dec >> 8).astype(F32)
    low = (dec & 255).astype(F32)
    steps = dt_ref[...].astype(F32)
    top = lax.broadcasted_iota(jnp.int32, (8, 128), 0) < HEADS
    for j in range(D // PACK_STEPS):
        group = slice(N * (j // 4), N * (j // 4 + 1))
        for half in range(2):
            cols = slice(LANES * j + 128 * half, LANES * j + 128 * (half + 1))
            out_ref[j, X_AT + T * half : X_AT + T * (half + 1)] = x_ref[:, cols]
            out_ref[j, UP_AT + T * half : UP_AT + T * (half + 1)] = up_ref[:, cols]
        out_ref[j, WRITE_AT : WRITE_AT + T] = write_ref[:, group]
        out_ref[j, READ_AT : READ_AT + T] = read_ref[:, group]
        base = 8 * (j // 2)
        steps8, high8, low8 = (rows[base : base + 8] for rows in (steps, high, low))
        if j % 2 == 1:
            steps8, low8 = pltpu.roll(steps8, HEADS, 0), pltpu.roll(low8, HEADS, 0)
        else:
            high8 = pltpu.roll(high8, HEADS, 0)
        tail = jnp.concatenate([jnp.where(top, steps8, high8), low8], axis=0)
        out_ref[j, TAIL_AT:ROWS] = tail.astype(BF16)


def wide(ref, b, at):
    return jnp.concatenate([ref[b, at : at + T], ref[b, at + T : at + 2 * T]], axis=1).astype(F32)


def thirds(rows):
    high = rows.astype(BF16).astype(F32)
    middle = (rows - high).astype(BF16).astype(F32)
    return high, middle, rows - high - middle


def prepare(tail_ref, held):
    upto = (
        lax.broadcasted_iota(jnp.int32, (T, T), 0) <= lax.broadcasted_iota(jnp.int32, (T, T), 1)
    ).astype(F32).astype(BF16)
    tail = tail_ref[...].reshape(2 * T, T)
    sums = contract(tail, upto, ((1,), (0,))).reshape(D, 2, 8, T)
    step = tail.astype(F32).reshape(D, 2, 8, T)[:, 0].reshape(T, T) / 16.0
    whole = pltpu.roll(sums[:, 0].reshape(T, T), T - HEADS, 0) * 256.0 + sums[:, 1].reshape(T, T)
    log_decay = -(whole / 65536.0)
    last = jnp.broadcast_to(log_decay[:, T - 1 : T], (T, T))
    ending = jnp.exp(last - log_decay) * step
    block_decay = jnp.exp(last).astype(BF16).astype(F32)
    pieces = (*thirds(log_decay), *thirds(ending), *thirds(jnp.exp(log_decay)), step, block_decay)
    for n, rows in enumerate(pieces):
        held[n] = rows


def kept(held, block):
    rows = pl.ds(pl.multiple_of(8 * block, 8), 8)
    got = [held[n, rows, :] for n in range(HELD)]
    return got[:3], got[3:6], got[6:9], got[9], got[10]


def head_marks(rows, width):
    row = lax.broadcasted_iota(jnp.int32, (rows, HEADS * width), 0) % 8
    lane = lax.broadcasted_iota(jnp.int32, (rows, HEADS * width), 1) // width
    return (row == lane).astype(F32)


def gaps(parts, marks):
    place = lax.broadcasted_iota(jnp.int32, (8, T), 0)
    minus = []
    for j in range(HEADS):
        tile = jnp.zeros((8, T), F32)
        for n, part in enumerate(parts):
            tile = jnp.where(place == n, -part[j : j + 1], tile)
        minus.append(tile)
    left = jnp.concatenate([*parts, jnp.ones((8, T), F32)], axis=0).astype(BF16)
    right = jnp.concatenate([marks, jnp.concatenate(minus, axis=1)], axis=0).astype(BF16)
    return contract(left, right, ((0,), (0,)))


def spread(parts, marks):
    return contract(jnp.concatenate(parts, axis=0).astype(BF16), marks, ((0,), (0,)))


def low_half(shape):
    return lax.broadcasted_iota(jnp.int32, shape, len(shape) - 1) < P_SIZE


def spread_rows(rows):
    mask = low_half((1, 128))
    return jnp.concatenate(
        [
            jnp.where(mask, rows[2 * i : 2 * i + 1], rows[2 * i + 1 : 2 * i + 2])
            for i in range(HEADS // 2)
        ],
        axis=1,
    )


def skip_lanes(skip_ref):
    lane = lax.broadcasted_iota(jnp.int32, (1, LANES), 1) // P_SIZE
    row = jnp.full((1, LANES), skip_ref[HEADS - 1], F32)
    for j in range(HEADS - 1):
        row = jnp.where(lane == j, skip_ref[j], row)
    return row


def two_heads(pair):
    mask = low_half((T, 128))
    return jnp.concatenate(
        [jnp.where(mask, pair, 0.0).astype(BF16), jnp.where(mask, 0.0, pair).astype(BF16)], axis=0
    )


def forward_kernel(
    in_ref, tail_ref, gain_ref, skip_ref, mo_ref, carried_ref, stats_ref, carry, sums, held
):
    step_id = pl.program_id(0)

    @pl.when(step_id == 0)
    def _():
        carry[...] = jnp.zeros_like(carry)
        sums[...] = jnp.zeros_like(sums)
        prepare(tail_ref, held)

    gain = gain_ref[...]
    skip = skip_lanes(skip_ref)
    row_id = lax.broadcasted_iota(jnp.int32, (T, T), 0)
    lane_id = lax.broadcasted_iota(jnp.int32, (T, T), 1)
    causal = row_id >= lane_id
    marks = head_marks(24, P_SIZE).astype(BF16)
    wide_marks = head_marks(24, T)
    state = carry[...]
    found = sums[...]
    results = []
    for b in range(BLOCKS_PER_STEP):
        x = wide(in_ref, b, X_AT)
        up = wide(in_ref, b, UP_AT)
        write = in_ref[b, WRITE_AT : WRITE_AT + T]
        read = in_ref[b, READ_AT : READ_AT + T]
        at = BLOCKS_PER_STEP * step_id + b
        decays, ending, readout, step, block_decay = kept(held, at)
        gap = gaps(decays, wide_marks)
        ending, readout = spread(ending, marks), spread(readout, marks)
        scores = contract(read, write, ((1,), (1,)))
        inner = []
        for i in range(HEADS // 2):
            mixing = []
            for j in (2 * i, 2 * i + 1):
                decay = jnp.exp(jnp.where(causal, gap[:, T * j : T * (j + 1)], FAR))
                mixing.append((scores * (decay * step[j : j + 1])).astype(BF16))
            inner.append(
                contract(
                    jnp.concatenate(mixing, axis=1),
                    two_heads(x[:, 128 * i : 128 * (i + 1)]),
                    ((1,), (0,)),
                )
            )
        weighted = (x * ending).astype(BF16)
        span_state = contract(write, weighted, ((0,), (0,))).astype(BF16).astype(F32)
        carried = state.astype(BF16)
        state = (spread_rows(block_decay) * state + span_state).astype(BF16).astype(F32)
        out = (
            jnp.concatenate(inner, axis=1)
            + readout * contract(read, carried, ((1,), (0,)))
            + skip * x
        )
        square = jnp.sum(out * out, axis=1, keepdims=True)
        cross = jnp.sum(up * gain * out, axis=1, keepdims=True)
        found = jnp.where(lane_id == at, square, jnp.where(lane_id == D + at, cross, found))
        results.append((out, carried))
    for b, (out, carried) in enumerate(results):
        mo_ref[b] = out
        carried_ref[b] = carried
    carry[...] = state
    sums[...] = found

    @pl.when(step_id == STEPS - 1)
    def _():
        rows = jnp.transpose(sums[...])[: 2 * D]
        for d in range(4):
            stats_ref[d] = rows


def shared_sums(stats_ref, sums):
    total = stats_ref[0] + stats_ref[1] + stats_ref[2] + stats_ref[3]
    inverse = lax.rsqrt(total[:D] / (HG * P_SIZE) + 1e-05)
    mean = inverse * total[D:] / (HG * P_SIZE)
    for n, part in enumerate((*thirds(inverse), *thirds(mean))):
        sums[n] = part


def normalise(sums, block, out, up, gain):
    place = lax.broadcasted_iota(jnp.int32, (8, T), 0)
    rows = jnp.zeros((8, T), F32)
    for n in range(6):
        rows = jnp.where(place == n, sums[n, pl.ds(block, 1), :], rows)
    row = lax.broadcasted_iota(jnp.int32, (8, 2 * LANES), 0) // 3
    lane = lax.broadcasted_iota(jnp.int32, (8, 2 * LANES), 1) // LANES
    both = contract(rows.astype(BF16), (row == lane).astype(F32).astype(BF16), ((0,), (0,)))
    inverse, mean = both[:, :LANES], both[:, LANES:]
    normed = out * inverse
    return normed, inverse * (up * gain - normed * mean)


def gain_kernel(in_ref, mo_ref, stats_ref, gain_ref, part_ref, sums, parts):
    step_id = pl.program_id(0)

    @pl.when(step_id == 0)
    def _():
        parts[...] = jnp.zeros_like(parts)
        shared_sums(stats_ref, sums)

    gain = gain_ref[...]
    gain_sum = parts[0]
    skip_sum = parts[1]
    for b in range(GAIN_BLOCKS):
        x = wide(in_ref, b, X_AT)
        up = wide(in_ref, b, UP_AT)
        normed, delta = normalise(sums, GAIN_BLOCKS * step_id + b, mo_ref[b], up, gain)
        gain_sum = gain_sum + jnp.sum((up * normed).reshape(T // 8, 8, LANES), axis=0)
        skip_sum = skip_sum + jnp.sum((delta * x).reshape(T // 8, 8, LANES), axis=0)
    parts[0] = gain_sum
    parts[1] = skip_sum

    @pl.when(step_id == D // GAIN_BLOCKS - 1)
    def _():
        total = jnp.concatenate(
            [jnp.sum(parts[0], axis=0, keepdims=True), jnp.sum(parts[1], axis=0, keepdims=True)],
            axis=0,
        )
        for copy in range(part_ref.shape[0]):
            part_ref[copy] = total


def backward_kernel(
    in_ref,
    tail_ref,
    mo_ref,
    carried_ref,
    stats_ref,
    gain_ref,
    skip_ref,
    out_ref,
    carry,
    sums,
    held,
):
    step_id = pl.program_id(0)

    @pl.when(step_id == 0)
    def _():
        carry[...] = jnp.zeros_like(carry)
        shared_sums(stats_ref, sums)
        prepare(tail_ref, held)

    gain = gain_ref[...]
    skip = skip_lanes(skip_ref)
    row_id = lax.broadcasted_iota(jnp.int32, (T, T), 0)
    lane_id = lax.broadcasted_iota(jnp.int32, (T, T), 1)
    later = row_id <= lane_id
    marks = head_marks(24, P_SIZE).astype(BF16)
    wide_marks = head_marks(24, T)
    step_marks = head_marks(8, T).astype(BF16)
    state = carry[...]
    results = []
    first = BLOCKS_PER_STEP * (STEPS - 1 - step_id)
    for b in reversed(range(BLOCKS_PER_STEP)):
        x = wide(in_ref, b, X_AT)
        up = wide(in_ref, b, UP_AT)
        write = in_ref[b, WRITE_AT : WRITE_AT + T]
        read = in_ref[b, READ_AT : READ_AT + T]
        out = mo_ref[b]
        decays, ending, readout, step, block_decay = kept(held, first + b)
        gap = gaps(decays, wide_marks)
        ending, readout = spread(ending, marks), spread(readout, marks)
        step = spread([step], step_marks)
        _, delta = normalise(sums, first + b, out, up, gain)
        scaled = (delta * readout).astype(BF16)
        half = delta.astype(BF16)
        scores = contract(write, read, ((1,), (1,)))
        score_grad = jnp.zeros((T, T), F32)
        mixed = []
        for i in range(HEADS // 2):
            pair = slice(128 * i, 128 * (i + 1))
            mix_grad = contract(two_heads(x[:, pair]), half[:, pair], ((1,), (1,)))
            mixing = []
            for n, j in enumerate((2 * i, 2 * i + 1)):
                lanes = slice(T * j, T * (j + 1))
                weight = jnp.exp(jnp.where(later, -gap[:, lanes], FAR)) * step[:, lanes]
                mixing.append((scores * weight).astype(BF16))
                score_grad = score_grad + weight * mix_grad[T * n : T * (n + 1)]
            mixed.append(
                contract(
                    jnp.concatenate(mixing, axis=1), two_heads(delta[:, pair]), ((1,), (0,))
                )
            )
        carried_grad = state.astype(BF16)
        mixer_grad = (
            jnp.concatenate(mixed, axis=1)
            + ending * contract(write, carried_grad, ((1,), (0,)))
            + skip * delta
        )
        read_grad = contract(score_grad.astype(BF16), write, ((0,), (0,))) + contract(
            scaled, carried_ref[b], ((1,), (1,))
        )
        state_grad = contract(read, scaled, ((0,), (0,))).astype(BF16).astype(F32)
        state = (state_grad + spread_rows(block_decay) * state).astype(BF16).astype(F32)
        results.append((b, mixer_grad, read_grad))
    for b, mixer_grad, read_grad in results:
        mixer_grad = mixer_grad.astype(BF16)
        out_ref[b, :T] = mixer_grad[:, :128]
        out_ref[b, T : 2 * T] = mixer_grad[:, 128:]
        out_ref[b, 2 * T :] = read_grad.astype(BF16)
    carry[...] = state


def unpack_kernel(in_ref, mixer_ref, read_ref):
    for g in range(G):
        total = jnp.zeros((T, N), F32)
        for d in range(4 * g, 4 * g + 4):
            for half in range(2):
                at = LANES * d + 128 * half
                mixer_ref[:, at : at + 128] = in_ref[d, T * half : T * (half + 1)]
            total = total + in_ref[d, 2 * T :].astype(F32)
        read_ref[:, N * g : N * (g + 1)] = total.astype(BF16)


def whole(shape):
    return pl.BlockSpec(shape, lambda i: (0,) * len(shape))


TAILS = pl.BlockSpec((D, ROWS - TAIL_AT, 128), lambda i: (0, TAIL_AT // (ROWS - TAIL_AT), 0))
SCALARS = pl.BlockSpec(memory_space=pltpu.SMEM)


def call(kernel, grid, in_specs, out_specs, out_shape, scratch=(), flops=0, interpret=False):
    return pl.pallas_call(
        kernel,
        grid=(grid,),
        in_specs=in_specs,
        out_specs=out_specs,
        out_shape=out_shape,
        scratch_shapes=scratch,
        cost_estimate=pl.CostEstimate(flops=flops, bytes_accessed=1 << 20, transcendentals=0),
        interpret=interpret,
    )


def shape(dims, dtype):
    return jax.ShapeDtypeStruct(dims, dtype)


def build(interpret):
    def mixer(mixer_in, write_proj, read_proj, dt_steps, decay_exp, norm_gain, skip_gain, out_grad):
        def exchange(array, axes):
            return lax.all_to_all(array, axes, split_axis=0, concat_axis=0, tiled=True)

        gain = norm_gain.reshape(1, LANES)
        column = lambda i: (0, i)
        sent = call(
            pack_kernel,
            PACK_STEPS,
            [
                pl.BlockSpec((T, H * P_SIZE // PACK_STEPS), column),
                pl.BlockSpec((T, H * P_SIZE // PACK_STEPS), column),
                pl.BlockSpec((T, G * N // PACK_STEPS), column),
                pl.BlockSpec((T, G * N // PACK_STEPS), column),
                pl.BlockSpec((H // PACK_STEPS, T), lambda i: (i, 0)),
                pl.BlockSpec((H // PACK_STEPS, T), lambda i: (i, 0)),
            ],
            pl.BlockSpec((D // PACK_STEPS, ROWS, 128), lambda i: (i, 0, 0)),
            shape((D, ROWS, 128), BF16),
            interpret=interpret,
        )(
            mixer_in[0],
            out_grad[0],
            write_proj[0],
            read_proj[0],
            jnp.transpose(dt_steps[0]),
            jnp.transpose(decay_exp[0]),
        )
        blocks = exchange(sent, SEQ)

        along = lambda i: (i, 0, 0)
        size = BLOCKS_PER_STEP
        mixer_out, carried, stats = call(
            forward_kernel,
            STEPS,
            [pl.BlockSpec((size, TAIL_AT, 128), along), TAILS, whole((1, LANES)), SCALARS],
            [
                pl.BlockSpec((size, T, LANES), along),
                pl.BlockSpec((size, N, LANES), along),
                whole((4, 2 * D, T)),
            ],
            [
                shape((D, T, LANES), F32),
                shape((D, N, LANES), BF16),
                shape((4, 2 * D, T), F32),
            ],
            [
                pltpu.VMEM((N, LANES), F32),
                pltpu.VMEM((T, T), F32),
                pltpu.VMEM((HELD, T, T), F32),
            ],
            interpret=interpret,
        )(blocks, blocks, gain, skip_gain)
        stats = exchange(stats, "seq_1")

        near = lax.axis_size(NEAR)
        copies = call(
            gain_kernel,
            D // GAIN_BLOCKS,
            [
                pl.BlockSpec((GAIN_BLOCKS, WRITE_AT, 128), along),
                pl.BlockSpec((GAIN_BLOCKS, T, LANES), along),
                whole((4, 2 * D, T)),
                whole((1, LANES)),
            ],
            whole((near, 2, LANES)),
            shape((near, 2, LANES), F32),
            [pltpu.VMEM((6, D, T), F32), pltpu.VMEM((2, 8, LANES), F32)],
            interpret=interpret,
        )(blocks, mixer_out, stats, gain)
        parts = exchange(copies, NEAR) if near > 1 else copies
        back = lambda i: (STEPS - 1 - i, 0, 0)
        grads = call(
            backward_kernel,
            STEPS,
            [
                pl.BlockSpec((size, TAIL_AT, 128), back),
                TAILS,
                pl.BlockSpec((size, T, LANES), back),
                pl.BlockSpec((size, N, LANES), back),
                whole((4, 2 * D, T)),
                whole((1, LANES)),
                SCALARS,
            ],
            pl.BlockSpec((size, 3 * T, 128), back),
            shape((D, 3 * T, 128), BF16),
            [
                pltpu.VMEM((N, LANES), F32),
                pltpu.VMEM((6, D, T), F32),
                pltpu.VMEM((HELD, T, T), F32),
            ],
            flops=1 << 34,
            interpret=interpret,
        )(blocks, blocks, mixer_out, carried, stats, gain, skip_gain)
        grads = exchange(grads, SEQ)
        parts = jnp.sum(parts, axis=0)
        if lax.axis_size("z_high") == 4:
            one, two, three = (
                lax.ppermute(parts, "z_high", [(i, i ^ d) for i in range(4)]) for d in (1, 2, 3)
            )
            parts = (parts + one) + (two + three)
        mixer_grad, read_grad = pl.pallas_call(
            unpack_kernel,
            out_shape=[shape((T, H * P_SIZE), BF16), shape((T, G * N), BF16)],
            interpret=interpret,
        )(grads)
        return (
            mixer_grad[None],
            read_grad[None],
            parts[0],
            jnp.sum(parts[1].reshape(HEADS, P_SIZE), axis=1),
        )

    return mixer


def sharded(mesh, interpret=False):
    rep = ("z_high", "z_low", "core")
    big = P(rep, SEQ, None)
    return jax.shard_map(
        build(interpret),
        mesh=mesh,
        in_specs=(big, big, big, big, big, P(SEQ), P(SEQ), big),
        out_specs=(big, big, P(SEQ), P(SEQ)),
        check_vma=False,
    )


def solution(mesh):
    names = ("seq_0", "seq_1", "z_high", "z_low", "core")
    step = sharded(Mesh(mesh.devices.reshape(4, 4, 4, 8, 2), names))
    return step
```

```python
import jax
import jax.numpy as jnp
from jax import lax
from jax.experimental import pallas as pl
from jax.experimental.pallas import tpu as pltpu
from jax.sharding import Mesh
from jax.sharding import PartitionSpec as P


H = 64
P_SIZE = 64
N = 128
G = 4
HG = 16
T = 128
D = 16
HEADS = H // D
LANES = HEADS * P_SIZE
SEQ = ("seq_0", "seq_1")
NEAR = ("z_low", "core")
F32 = jnp.float32
BF16 = jnp.bfloat16
BLOCKS_PER_STEP = 4
STEPS = D // BLOCKS_PER_STEP
PACK_STEPS = 2
GAIN_BLOCKS = 8
FAR = -1e30
HELD = 11
X_AT, UP_AT, WRITE_AT, READ_AT, TAIL_AT, ROWS = 0, 256, 512, 640, 768, 784


def contract(left, right, dims):
    return lax.dot_general(left, right, (dims, ((), ())), preferred_element_type=F32)


def pack_kernel(x_ref, up_ref, write_ref, read_ref, dt_ref, dec_ref, out_ref):
    dec = dec_ref[...]
    high = (dec >> 8).astype(F32)
    low = (dec & 255).astype(F32)
    steps = dt_ref[...].astype(F32)
    top = lax.broadcasted_iota(jnp.int32, (8, 128), 0) < HEADS
    for j in range(D // PACK_STEPS):
        group = slice(N * (j // 4), N * (j // 4 + 1))
        for half in range(2):
            cols = slice(LANES * j + 128 * half, LANES * j + 128 * (half + 1))
            out_ref[j, X_AT + T * half : X_AT + T * (half + 1)] = x_ref[:, cols]
            out_ref[j, UP_AT + T * half : UP_AT + T * (half + 1)] = up_ref[:, cols]
        out_ref[j, WRITE_AT : WRITE_AT + T] = write_ref[:, group]
        out_ref[j, READ_AT : READ_AT + T] = read_ref[:, group]
        base = 8 * (j // 2)
        steps8, high8, low8 = (rows[base : base + 8] for rows in (steps, high, low))
        if j % 2 == 1:
            steps8, low8 = pltpu.roll(steps8, HEADS, 0), pltpu.roll(low8, HEADS, 0)
        else:
            high8 = pltpu.roll(high8, HEADS, 0)
        tail = jnp.concatenate([jnp.where(top, steps8, high8), low8], axis=0)
        out_ref[j, TAIL_AT:ROWS] = tail.astype(BF16)


def wide(ref, b, at):
    return jnp.concatenate([ref[b, at : at + T], ref[b, at + T : at + 2 * T]], axis=1).astype(F32)


def thirds(rows):
    high = rows.astype(BF16).astype(F32)
    middle = (rows - high).astype(BF16).astype(F32)
    return high, middle, rows - high - middle


def prepare(tail_ref, held):
    upto = (
        lax.broadcasted_iota(jnp.int32, (T, T), 0) <= lax.broadcasted_iota(jnp.int32, (T, T), 1)
    ).astype(F32).astype(BF16)
    tail = tail_ref[...].reshape(2 * T, T)
    sums = contract(tail, upto, ((1,), (0,))).reshape(D, 2, 8, T)
    step = tail.astype(F32).reshape(D, 2, 8, T)[:, 0].reshape(T, T) / 16.0
    whole = pltpu.roll(sums[:, 0].reshape(T, T), T - HEADS, 0) * 256.0 + sums[:, 1].reshape(T, T)
    log_decay = -(whole / 65536.0)
    last = jnp.broadcast_to(log_decay[:, T - 1 : T], (T, T))
    ending = jnp.exp(last - log_decay) * step
    block_decay = jnp.exp(last).astype(BF16).astype(F32)
    pieces = (*thirds(log_decay), *thirds(ending), *thirds(jnp.exp(log_decay)), step, block_decay)
    for n, rows in enumerate(pieces):
        held[n] = rows


def kept(held, block):
    rows = pl.ds(pl.multiple_of(8 * block, 8), 8)
    got = [held[n, rows, :] for n in range(HELD)]
    return got[:3], got[3:6], got[6:9], got[9], got[10]


def head_marks(rows, width):
    row = lax.broadcasted_iota(jnp.int32, (rows, HEADS * width), 0) % 8
    lane = lax.broadcasted_iota(jnp.int32, (rows, HEADS * width), 1) // width
    return (row == lane).astype(F32)


def gaps(parts, marks):
    place = lax.broadcasted_iota(jnp.int32, (8, T), 0)
    minus = []
    for j in range(HEADS):
        tile = jnp.zeros((8, T), F32)
        for n, part in enumerate(parts):
            tile = jnp.where(place == n, -part[j : j + 1], tile)
        minus.append(tile)
    left = jnp.concatenate([*parts, jnp.ones((8, T), F32)], axis=0).astype(BF16)
    right = jnp.concatenate([marks, jnp.concatenate(minus, axis=1)], axis=0).astype(BF16)
    return contract(left, right, ((0,), (0,)))


def spread(parts, marks):
    return contract(jnp.concatenate(parts, axis=0).astype(BF16), marks, ((0,), (0,)))


def low_half(shape):
    return lax.broadcasted_iota(jnp.int32, shape, len(shape) - 1) < P_SIZE


def spread_rows(rows):
    mask = low_half((1, 128))
    return jnp.concatenate(
        [
            jnp.where(mask, rows[2 * i : 2 * i + 1], rows[2 * i + 1 : 2 * i + 2])
            for i in range(HEADS // 2)
        ],
        axis=1,
    )


def skip_lanes(skip_ref):
    lane = lax.broadcasted_iota(jnp.int32, (1, LANES), 1) // P_SIZE
    row = jnp.full((1, LANES), skip_ref[HEADS - 1], F32)
    for j in range(HEADS - 1):
        row = jnp.where(lane == j, skip_ref[j], row)
    return row


def two_heads(pair):
    mask = low_half((T, 128))
    return jnp.concatenate(
        [jnp.where(mask, pair, 0.0).astype(BF16), jnp.where(mask, 0.0, pair).astype(BF16)], axis=0
    )


def forward_kernel(
    in_ref, tail_ref, gain_ref, skip_ref, mo_ref, carried_ref, stats_ref, carry, sums, held
):
    step_id = pl.program_id(0)

    @pl.when(step_id == 0)
    def _():
        carry[...] = jnp.zeros_like(carry)
        sums[...] = jnp.zeros_like(sums)
        prepare(tail_ref, held)

    gain = gain_ref[...]
    skip = skip_lanes(skip_ref)
    row_id = lax.broadcasted_iota(jnp.int32, (T, T), 0)
    lane_id = lax.broadcasted_iota(jnp.int32, (T, T), 1)
    causal = row_id >= lane_id
    marks = head_marks(24, P_SIZE).astype(BF16)
    wide_marks = head_marks(24, T)
    state = carry[...]
    found = sums[...]
    results = []
    for b in range(BLOCKS_PER_STEP):
        x = wide(in_ref, b, X_AT)
        up = wide(in_ref, b, UP_AT)
        write = in_ref[b, WRITE_AT : WRITE_AT + T]
        read = in_ref[b, READ_AT : READ_AT + T]
        at = BLOCKS_PER_STEP * step_id + b
        decays, ending, readout, step, block_decay = kept(held, at)
        gap = gaps(decays, wide_marks)
        ending, readout = spread(ending, marks), spread(readout, marks)
        scores = contract(read, write, ((1,), (1,)))
        inner = []
        for i in range(HEADS // 2):
            mixing = []
            for j in (2 * i, 2 * i + 1):
                decay = jnp.exp(jnp.where(causal, gap[:, T * j : T * (j + 1)], FAR))
                mixing.append((scores * (decay * step[j : j + 1])).astype(BF16))
            inner.append(
                contract(
                    jnp.concatenate(mixing, axis=1),
                    two_heads(x[:, 128 * i : 128 * (i + 1)]),
                    ((1,), (0,)),
                )
            )
        weighted = (x * ending).astype(BF16)
        span_state = contract(write, weighted, ((0,), (0,))).astype(BF16).astype(F32)
        carried = state.astype(BF16)
        state = (spread_rows(block_decay) * state + span_state).astype(BF16).astype(F32)
        out = (
            jnp.concatenate(inner, axis=1)
            + readout * contract(read, carried, ((1,), (0,)))
            + skip * x
        )
        square = jnp.sum(out * out, axis=1, keepdims=True)
        cross = jnp.sum(up * gain * out, axis=1, keepdims=True)
        found = jnp.where(lane_id == at, square, jnp.where(lane_id == D + at, cross, found))
        results.append((out, carried))
    for b, (out, carried) in enumerate(results):
        mo_ref[b] = out
        carried_ref[b] = carried
    carry[...] = state
    sums[...] = found

    @pl.when(step_id == STEPS - 1)
    def _():
        rows = jnp.transpose(sums[...])[: 2 * D]
        for d in range(4):
            stats_ref[d] = rows


def shared_sums(stats_ref, sums):
    total = stats_ref[0] + stats_ref[1] + stats_ref[2] + stats_ref[3]
    inverse = lax.rsqrt(total[:D] / (HG * P_SIZE) + 1e-05)
    mean = inverse * total[D:] / (HG * P_SIZE)
    for n, part in enumerate((*thirds(inverse), *thirds(mean))):
        sums[n] = part


def normalise(sums, block, out, up, gain):
    place = lax.broadcasted_iota(jnp.int32, (8, T), 0)
    rows = jnp.zeros((8, T), F32)
    for n in range(6):
        rows = jnp.where(place == n, sums[n, pl.ds(block, 1), :], rows)
    row = lax.broadcasted_iota(jnp.int32, (8, 2 * LANES), 0) // 3
    lane = lax.broadcasted_iota(jnp.int32, (8, 2 * LANES), 1) // LANES
    both = contract(rows.astype(BF16), (row == lane).astype(F32).astype(BF16), ((0,), (0,)))
    inverse, mean = both[:, :LANES], both[:, LANES:]
    normed = out * inverse
    return normed, inverse * (up * gain - normed * mean)


def gain_kernel(in_ref, mo_ref, stats_ref, gain_ref, part_ref, sums, parts):
    step_id = pl.program_id(0)

    @pl.when(step_id == 0)
    def _():
        parts[...] = jnp.zeros_like(parts)
        shared_sums(stats_ref, sums)

    gain = gain_ref[...]
    gain_sum = parts[0]
    skip_sum = parts[1]
    for b in range(GAIN_BLOCKS):
        x = wide(in_ref, b, X_AT)
        up = wide(in_ref, b, UP_AT)
        normed, delta = normalise(sums, GAIN_BLOCKS * step_id + b, mo_ref[b], up, gain)
        gain_sum = gain_sum + jnp.sum((up * normed).reshape(T // 8, 8, LANES), axis=0)
        skip_sum = skip_sum + jnp.sum((delta * x).reshape(T // 8, 8, LANES), axis=0)
    parts[0] = gain_sum
    parts[1] = skip_sum

    @pl.when(step_id == D // GAIN_BLOCKS - 1)
    def _():
        total = jnp.concatenate(
            [jnp.sum(parts[0], axis=0, keepdims=True), jnp.sum(parts[1], axis=0, keepdims=True)],
            axis=0,
        )
        for copy in range(part_ref.shape[0]):
            part_ref[copy] = total


def backward_kernel(
    in_ref,
    tail_ref,
    mo_ref,
    carried_ref,
    stats_ref,
    gain_ref,
    skip_ref,
    out_ref,
    carry,
    sums,
    held,
):
    step_id = pl.program_id(0)

    @pl.when(step_id == 0)
    def _():
        carry[...] = jnp.zeros_like(carry)
        shared_sums(stats_ref, sums)
        prepare(tail_ref, held)

    gain = gain_ref[...]
    skip = skip_lanes(skip_ref)
    row_id = lax.broadcasted_iota(jnp.int32, (T, T), 0)
    lane_id = lax.broadcasted_iota(jnp.int32, (T, T), 1)
    later = row_id <= lane_id
    marks = head_marks(24, P_SIZE).astype(BF16)
    wide_marks = head_marks(24, T)
    step_marks = head_marks(8, T).astype(BF16)
    state = carry[...]
    results = []
    first = BLOCKS_PER_STEP * (STEPS - 1 - step_id)
    for b in reversed(range(BLOCKS_PER_STEP)):
        x = wide(in_ref, b, X_AT)
        up = wide(in_ref, b, UP_AT)
        write = in_ref[b, WRITE_AT : WRITE_AT + T]
        read = in_ref[b, READ_AT : READ_AT + T]
        out = mo_ref[b]
        decays, ending, readout, step, block_decay = kept(held, first + b)
        gap = gaps(decays, wide_marks)
        ending, readout = spread(ending, marks), spread(readout, marks)
        step = spread([step], step_marks)
        _, delta = normalise(sums, first + b, out, up, gain)
        scaled = (delta * readout).astype(BF16)
        half = delta.astype(BF16)
        scores = contract(write, read, ((1,), (1,)))
        score_grad = jnp.zeros((T, T), F32)
        mixed = []
        for i in range(HEADS // 2):
            pair = slice(128 * i, 128 * (i + 1))
            mix_grad = contract(two_heads(x[:, pair]), half[:, pair], ((1,), (1,)))
            mixing = []
            for n, j in enumerate((2 * i, 2 * i + 1)):
                lanes = slice(T * j, T * (j + 1))
                weight = jnp.exp(jnp.where(later, -gap[:, lanes], FAR)) * step[:, lanes]
                mixing.append((scores * weight).astype(BF16))
                score_grad = score_grad + weight * mix_grad[T * n : T * (n + 1)]
            mixed.append(
                contract(
                    jnp.concatenate(mixing, axis=1), two_heads(delta[:, pair]), ((1,), (0,))
                )
            )
        carried_grad = state.astype(BF16)
        mixer_grad = (
            jnp.concatenate(mixed, axis=1)
            + ending * contract(write, carried_grad, ((1,), (0,)))
            + skip * delta
        )
        read_grad = contract(score_grad.astype(BF16), write, ((0,), (0,))) + contract(
            scaled, carried_ref[b], ((1,), (1,))
        )
        state_grad = contract(read, scaled, ((0,), (0,))).astype(BF16).astype(F32)
        state = (state_grad + spread_rows(block_decay) * state).astype(BF16).astype(F32)
        results.append((b, mixer_grad, read_grad))
    for b, mixer_grad, read_grad in results:
        mixer_grad = mixer_grad.astype(BF16)
        out_ref[b, :T] = mixer_grad[:, :128]
        out_ref[b, T : 2 * T] = mixer_grad[:, 128:]
        out_ref[b, 2 * T :] = read_grad.astype(BF16)
    carry[...] = state


def unpack_kernel(in_ref, mixer_ref, read_ref):
    for g in range(G // 2):
        total = jnp.zeros((T, N), F32)
        for d in range(4 * g, 4 * g + 4):
            for half in range(2):
                at = LANES * d + 128 * half
                mixer_ref[:, at : at + 128] = in_ref[d, T * half : T * (half + 1)]
            total = total + in_ref[d, 2 * T :].astype(F32)
        read_ref[:, N * g : N * (g + 1)] = total.astype(BF16)


def whole(shape):
    return pl.BlockSpec(shape, lambda i: (0,) * len(shape))


TAILS = pl.BlockSpec((D, ROWS - TAIL_AT, 128), lambda i: (0, TAIL_AT // (ROWS - TAIL_AT), 0))
SCALARS = pl.BlockSpec(memory_space=pltpu.SMEM)


def call(kernel, grid, in_specs, out_specs, out_shape, scratch=(), flops=0, interpret=False):
    return pl.pallas_call(
        kernel,
        grid=(grid,),
        in_specs=in_specs,
        out_specs=out_specs,
        out_shape=out_shape,
        scratch_shapes=scratch,
        cost_estimate=pl.CostEstimate(flops=flops, bytes_accessed=1 << 20, transcendentals=0),
        interpret=interpret,
    )


def shape(dims, dtype):
    return jax.ShapeDtypeStruct(dims, dtype)


def build(interpret):
    def mixer(mixer_in, write_proj, read_proj, dt_steps, decay_exp, norm_gain, skip_gain, out_grad):
        def exchange(array, axes):
            return lax.all_to_all(array, axes, split_axis=0, concat_axis=0, tiled=True)

        gain = norm_gain.reshape(1, LANES)
        column = lambda i: (0, i)
        sent = call(
            pack_kernel,
            PACK_STEPS,
            [
                pl.BlockSpec((T, H * P_SIZE // PACK_STEPS), column),
                pl.BlockSpec((T, H * P_SIZE // PACK_STEPS), column),
                pl.BlockSpec((T, G * N // PACK_STEPS), column),
                pl.BlockSpec((T, G * N // PACK_STEPS), column),
                pl.BlockSpec((H // PACK_STEPS, T), lambda i: (i, 0)),
                pl.BlockSpec((H // PACK_STEPS, T), lambda i: (i, 0)),
            ],
            pl.BlockSpec((D // PACK_STEPS, ROWS, 128), lambda i: (i, 0, 0)),
            shape((D, ROWS, 128), BF16),
            interpret=interpret,
        )(
            mixer_in[0],
            out_grad[0],
            write_proj[0],
            read_proj[0],
            jnp.transpose(dt_steps[0]),
            jnp.transpose(decay_exp[0]),
        )
        blocks = exchange(sent, SEQ)

        along = lambda i: (i, 0, 0)
        size = BLOCKS_PER_STEP
        mixer_out, carried, stats = call(
            forward_kernel,
            STEPS,
            [pl.BlockSpec((size, TAIL_AT, 128), along), TAILS, whole((1, LANES)), SCALARS],
            [
                pl.BlockSpec((size, T, LANES), along),
                pl.BlockSpec((size, N, LANES), along),
                whole((4, 2 * D, T)),
            ],
            [
                shape((D, T, LANES), F32),
                shape((D, N, LANES), BF16),
                shape((4, 2 * D, T), F32),
            ],
            [
                pltpu.VMEM((N, LANES), F32),
                pltpu.VMEM((T, T), F32),
                pltpu.VMEM((HELD, T, T), F32),
            ],
            interpret=interpret,
        )(blocks, blocks, gain, skip_gain)
        stats = exchange(stats, "seq_1")

        near = lax.axis_size(NEAR)
        copies = call(
            gain_kernel,
            D // GAIN_BLOCKS,
            [
                pl.BlockSpec((GAIN_BLOCKS, WRITE_AT, 128), along),
                pl.BlockSpec((GAIN_BLOCKS, T, LANES), along),
                whole((4, 2 * D, T)),
                whole((1, LANES)),
            ],
            whole((near, 2, LANES)),
            shape((near, 2, LANES), F32),
            [pltpu.VMEM((6, D, T), F32), pltpu.VMEM((2, 8, LANES), F32)],
            interpret=interpret,
        )(blocks, mixer_out, stats, gain)
        parts = exchange(copies, NEAR) if near > 1 else copies
        back = lambda i: (STEPS - 1 - i, 0, 0)
        grads = call(
            backward_kernel,
            STEPS,
            [
                pl.BlockSpec((size, TAIL_AT, 128), back),
                TAILS,
                pl.BlockSpec((size, T, LANES), back),
                pl.BlockSpec((size, N, LANES), back),
                whole((4, 2 * D, T)),
                whole((1, LANES)),
                SCALARS,
            ],
            pl.BlockSpec((size, 3 * T, 128), back),
            shape((D, 3 * T, 128), BF16),
            [
                pltpu.VMEM((N, LANES), F32),
                pltpu.VMEM((6, D, T), F32),
                pltpu.VMEM((HELD, T, T), F32),
            ],
            flops=1 << 34,
            interpret=interpret,
        )(blocks, blocks, mixer_out, carried, stats, gain, skip_gain)
        grads = exchange(grads, SEQ)
        parts = jnp.sum(parts, axis=0)
        if lax.axis_size("z_high") == 4:
            two, one, three = (
                lax.ppermute(parts, "z_high", [(i, i ^ d) for i in range(4)]) for d in (2, 1, 3)
            )
            parts = (parts + one) + (two + three)
        mixer_grad, read_grad = pl.pallas_call(
            unpack_kernel,
            grid=(2,),
            in_specs=[pl.BlockSpec((D // 2, 3 * T, 128), along)],
            out_specs=[pl.BlockSpec((T, H * P_SIZE // 2), column), pl.BlockSpec((T, G * N // 2), column)],
            out_shape=[shape((T, H * P_SIZE), BF16), shape((T, G * N), BF16)],
            interpret=interpret,
        )(grads)
        return (
            mixer_grad[None],
            read_grad[None],
            parts[0],
            jnp.sum(parts[1].reshape(HEADS, P_SIZE), axis=1),
        )

    return mixer


def sharded(mesh, interpret=False):
    rep = ("z_high", "z_low", "core")
    big = P(rep, SEQ, None)
    return jax.shard_map(
        build(interpret),
        mesh=mesh,
        in_specs=(big, big, big, big, big, P(SEQ), P(SEQ), big),
        out_specs=(big, big, P(SEQ), P(SEQ)),
        check_vma=False,
    )


def solution(mesh):
    names = ("seq_0", "seq_1", "z_high", "z_low", "core")
    step = sharded(Mesh(mesh.devices.reshape(4, 4, 4, 8, 2), names))
    return step
```
